128 devices in a mesh: rep: 2 (over core), dp: 64 (over x, y, z).
Axes of the slice: x: 4, y: 4, z: 4, core: 2. Of those that a mesh axis runs over, the one named last changes fastest.
Arguments:
- g_w_gate: bfloat16 [128, 2, 640, 3200], P(('rep', 'dp')), parts along dimension 0
- g_w_up: bfloat16 [128, 2, 640, 3200], P(('rep', 'dp')), parts along dimension 0
- g_w_down: bfloat16 [128, 2, 3200, 640], P(('rep', 'dp')), parts along dimension 0
- w_gate: bfloat16 [2, 640, 3200], replicated
- w_up: bfloat16 [2, 640, 3200], replicated
- w_down: bfloat16 [2, 3200, 640], replicated
- m_w_gate: float32 [2, 640, 3200], P(None, 'dp')
- m_w_up: float32 [2, 640, 3200], P(None, 'dp')
- m_w_down: float32 [2, 3200, 640], P(None, 'dp')
- v_w_gate: float32 [2, 640, 3200], P(None, 'dp')
- v_w_up: float32 [2, 640, 3200], P(None, 'dp')
- v_w_down: float32 [2, 3200, 640], P(None, 'dp')
Outputs:
- output 1: bfloat16 [4, 640, 3200], P('rep'), parts along dimension 0
- output 2: bfloat16 [4, 640, 3200], P('rep'), parts along dimension 0
- output 3: bfloat16 [4, 3200, 640], P('rep'), parts along dimension 0
- output 4: float32 [4, 640, 3200], P('rep', 'dp'), parts along dimension 0
- output 5: float32 [4, 640, 3200], P('rep', 'dp'), parts along dimension 0
- output 6: float32 [4, 3200, 640], P('rep', 'dp'), parts along dimension 0
- output 7: float32 [4, 640, 3200], P('rep', 'dp'), parts along dimension 0
- output 8: float32 [4, 640, 3200], P('rep', 'dp'), parts along dimension 0
- output 9: float32 [4, 3200, 640], P('rep', 'dp'), parts along dimension 0
There are 2 independent parts. The reference program is written for one: setup_inputs(seed, part) draws one part's arguments, and reference() takes and returns one part's arrays. A program takes and returns all parts, laid end to end along the dimension named above; an argument that names none is the same for every part.
All inputs are finite; a program needn't handle non-finite values.
Results may differ from the reference program's by a relative error of at most 0.022.
Values are sent between devices in bfloat16 or wider.
A program may use at most 1.5 GiB of HBM per device.

```python
import jax
import jax.numpy as jnp
from jax import lax

DEVICES = 64
D = 640
FF = 3200
LAYERS = 2
NAMES = ("w_gate", "w_up", "w_down")
SHAPES = {"w_gate": (LAYERS, D, FF), "w_up": (LAYERS, D, FF), "w_down": (LAYERS, FF, D)}


def setup_inputs(seed: int = 0, part: int = 0) -> dict:
    kz, *keys = jax.random.split(jax.random.key(seed), 1 + 5 * len(NAMES))
    loud = 2.0 ** jax.random.uniform(kz, (), jnp.float32, -1.0, 1.0)
    drawn = {}
    for name, key, both in zip(NAMES, keys[:3], keys[3:6], strict=True):
        own = jax.random.normal(jax.random.fold_in(key, part), (DEVICES, *SHAPES[name]), jnp.float32)
        shared = jax.random.normal(jax.random.fold_in(both, part), SHAPES[name], jnp.float32)
        drawn["g_" + name] = (loud * (0.7 * shared / DEVICES + 0.7 * own * DEVICES**-0.5)).astype(jnp.bfloat16)
    for name, key in zip(NAMES, keys[6:9], strict=True):
        drawn[name] = (jax.random.normal(key, SHAPES[name], jnp.float32) * SHAPES[name][1] ** -0.5).astype(jnp.bfloat16)
    for name, key in zip(NAMES, keys[9:12], strict=True):
        drawn["m_" + name] = loud * 0.5 * jax.random.normal(key, SHAPES[name], jnp.float32)
    for name, key in zip(NAMES, keys[12:15], strict=True):
        drawn["v_" + name] = loud * loud * jax.random.uniform(key, SHAPES[name], jnp.float32, 0.5, 1.5)
    return drawn


def adamw(w, m, v, g):
    m = 0.9 * m + 0.1 * g
    v = 0.95 * v + 0.05 * g * g
    step = m * lax.rsqrt(v + 1e-8) + 0.1 * w
    return (w - 0.02 * step).astype(jnp.bfloat16), m, v


def clipped(gradients, sum_of_squares, count):
    factor = jnp.minimum(1.0, 0.5 * lax.rsqrt(sum_of_squares / count + 1e-30))
    return [g * factor for g in gradients]


def reference(g_w_gate, g_w_up, g_w_down, w_gate, w_up, w_down, m_w_gate, m_w_up, m_w_down, v_w_gate, v_w_up, v_w_down):
    def total(terms):
        return lax.scan(lambda so_far, term: (so_far + term.astype(jnp.float32), None), jnp.zeros(terms.shape[1:], jnp.float32), terms)[0]

    gradients = [total(terms).astype(jnp.bfloat16).astype(jnp.float32) for terms in (g_w_gate, g_w_up, g_w_down)]
    gradients = clipped(gradients, sum(jnp.sum(g * g) for g in gradients), sum(g.size for g in gradients))
    new = [
        adamw(w.astype(jnp.float32), m, v, g)
        for w, m, v, g in zip((w_gate, w_up, w_down), (m_w_gate, m_w_up, m_w_down), (v_w_gate, v_w_up, v_w_down), gradients, strict=True)
    ]
    return tuple(one[which] for which in range(3) for one in new)
```

```python
import functools

import jax
import jax.numpy as jnp
import numpy as np
from jax import lax
from jax.experimental import pallas as pl
from jax.experimental.pallas import tpu as pltpu
from jax.sharding import PartitionSpec as P

MESH = pl.DeviceIdType.MESH
BF, F32 = jnp.bfloat16, jnp.float32
ANY = pl.BlockSpec(memory_space=pl.ANY)
VM = pl.BlockSpec(memory_space=pltpu.VMEM)

CT, CD = 25, 5
GU, DN = 40, 104
ROWS = CT * GU + CD * DN
BASE = CT * GU
COUNT = 3 * 2 * 640 * 3200
PARTS = ((0, 512, (0, 1, 2)), (512, 496, (1, 2, 0)), (1008, 512, (2, 0, 1)))
H0 = 256
I0, I1, I2, I3, I4 = range(5)


def perm_gu():
    p = np.zeros((160, 160), np.float32)
    for z in range(4):
        for s in range(4):
            for r in range(10):
                p[z * 40 + s * 10 + r, s * 40 + z * 10 + r] = 1
    return p


def perm_dn():
    p = np.zeros((4 * DN, 400), np.float32)
    for z in range(4):
        for s in range(2):
            for r in range(50):
                p[z * DN + s * 50 + r, s * 200 + z * 50 + r] = 1
    return p


def dot(a, b):
    return jnp.dot(a, b, preferred_element_type=F32)


def pack_line(pg, pd, gate, up, down, out):
    d = jnp.concatenate([down[0].astype(F32), down[1].astype(F32)], axis=0).astype(BF)
    d = dot(pd, d)
    for c in range(0, CT, 2):
        n = min(2, CT - c) * 128
        cols = pl.ds(c * 128, n)
        x = jnp.concatenate([ref[s, :, cols].astype(F32) for ref in (gate, up) for s in range(2)], axis=0).astype(BF)
        y = dot(pg, x)
        for z in range(4):
            one = [y[z * GU : (z + 1) * GU, i : i + 128] for i in range(0, n, 128)]
            if c == CT - 1:
                one.append(d[z * DN : (z + 1) * DN, 0:128])
            one = jnp.concatenate(one, axis=0).astype(BF)
            out[z, c * GU : c * GU + one.shape[0], :] = one
    for c in (1, 3):
        for z in range(4):
            one = [d[z * DN : (z + 1) * DN, i * 128 : (i + 1) * 128] for i in (c, c + 1)]
            out[z, BASE + c * DN : BASE + (c + 2) * DN, :] = jnp.concatenate(one, axis=0).astype(BF)


def pack_kernel(pg_ref, pd_ref, gate, up, down, out):
    pack_line(pg_ref[...], pd_ref[...], gate, up, down, out.at[0])


def pack(pg, pd, gate, up, down):
    lines = gate.shape[1] // 40
    whole = lambda a: pl.BlockSpec(a.shape, lambda i: (0,) * a.ndim)
    return pl.pallas_call(
        pack_kernel,
        grid=(lines,),
        out_shape=jax.ShapeDtypeStruct((lines, 4, ROWS, 128), BF),
        in_specs=[whole(pg), whole(pd)]
        + [pl.BlockSpec((2, 40, 3200), lambda i: (0, i, 0))] * 2
        + [pl.BlockSpec((2, 200, 640), lambda i: (0, i, 0))],
        out_specs=pl.BlockSpec((1, 4, ROWS, 128), lambda i: (i, 0, 0, 0)),
        name="pack",
    )(pg, pd, gate, up, down)


def moments_in_kernel(*refs):
    for refs3, out in ((refs[:3], refs[6]), (refs[3:6], refs[7])):
        out[...] = jnp.zeros_like(out)
        for w in range(2):
            for c in range(CT):
                for s in range(2):
                    out[pl.ds(c * GU + w * 20 + s * 10, 10), :] = refs3[w][pl.ds(2 * c + s, 10, stride=2 * CT), :]
        for c in range(CD):
            for s in range(2):
                out[pl.ds(BASE + c * DN + s * 50, 50), :] = refs3[2][pl.ds(2 * c + s, 50, stride=2 * CD), :]


def moments_in(flat):
    return pl.pallas_call(
        moments_in_kernel,
        out_shape=[jax.ShapeDtypeStruct((ROWS, 128), F32)] * 2,
        in_specs=[VM] * 6,
        out_specs=[VM] * 2,
        name="moments_in",
    )(*flat)


def moments_out(m, v, outs):
    for one, refs3 in ((m, outs[:3]), (v, outs[3:])):
        for w in range(2):
            for c in range(CT):
                for s in range(2):
                    refs3[w][pl.ds(2 * c + s, 10, stride=2 * CT), :] = one[pl.ds(c * GU + w * 20 + s * 10, 10), :]
        for c in range(CD):
            for s in range(2):
                refs3[2][pl.ds(2 * c + s, 50, stride=2 * CD), :] = one[pl.ds(BASE + c * DN + s * 50, 50), :]


def unpack_kernel(pg_ref, pd_ref, packed, m, v, gate, up, down, *outs):
    @pl.when(pl.program_id(0) == 0)
    def _():
        moments_out(m, v, outs)

    pg, pd = pg_ref[...], pd_ref[...]
    ds = [[] for _ in range(CD)]
    for c in range(0, CT, 2):
        n = min(2, CT - c)
        extra = DN if n == 1 else 0
        got = [packed[0, z, c * GU : c * GU + n * GU + extra, :].astype(F32) for z in range(4)]
        x = [jnp.concatenate([one[i * GU : (i + 1) * GU] for one in got], axis=0) for i in range(n)]
        x = jnp.concatenate(x, axis=1) if n == 2 else x[0]
        y = dot(pg, x.astype(BF))
        for i, (ref, s) in enumerate(((gate, 0), (gate, 1), (up, 0), (up, 1))):
            ref[s, :, c * 128 : (c + n) * 128] = y[i * 40 : (i + 1) * 40].astype(BF)
        if extra:
            ds[0] = [one[GU:] for one in got]
    for c in (1, 3):
        got = [packed[0, z, BASE + c * DN : BASE + (c + 2) * DN, :].astype(F32) for z in range(4)]
        for i in range(2):
            ds[c + i] = [one[i * DN : (i + 1) * DN] for one in got]
    for c in range(CD):
        y = dot(pd, jnp.concatenate(ds[c], axis=0).astype(BF))
        for s in range(2):
            down[s, :, c * 128 : (c + 1) * 128] = y[s * 200 : (s + 1) * 200].astype(BF)


def unpack(pg, pd, packed, m, v):
    whole = lambda a: pl.BlockSpec(a.shape, lambda i: (0,) * a.ndim)
    flat = pl.BlockSpec((500, 128), lambda i: (0, 0))
    return pl.pallas_call(
        unpack_kernel,
        grid=(16,),
        out_shape=[jax.ShapeDtypeStruct((2, 640, 3200), BF)] * 2
        + [jax.ShapeDtypeStruct((2, 3200, 640), BF)]
        + [jax.ShapeDtypeStruct((500, 128), F32)] * 6,
        in_specs=[whole(pg), whole(pd), pl.BlockSpec((1, 4, ROWS, 128), lambda i: (i, 0, 0, 0)), whole(m), whole(v)],
        out_specs=[pl.BlockSpec((2, 40, 3200), lambda i: (0, i, 0))] * 2
        + [pl.BlockSpec((2, 200, 640), lambda i: (0, i, 0))]
        + [flat] * 6,
        name="unpack",
    )(pg, pd, packed, m, v)


class Part:
    pass


def step_kernel(pk, wo, m, v, wg, mo, vo, wn, gs, sq, sqr, *rest):
    bufs, sems = rest[: 3 * PART_BUFS], rest[3 * PART_BUFS :]
    recv, send, local, one_sem = sems
    rep, dp = lax.axis_index("rep"), lax.axis_index("dp")
    here = [lax.div(dp, 16), lax.rem(lax.div(dp, 4), 4), lax.rem(dp, 4)]

    def at(axis, by):
        return lax.rem(here[axis] + by + 4, 4)

    def device(axis, by):
        c = list(here)
        c[axis] = at(axis, by)
        return (rep, c[I0] * 16 + c[I1] * 4 + c[I2])

    barrier = pltpu.get_barrier_semaphore()
    for axis in range(3):
        for by in (1, 2, 3):
            pl.semaphore_signal(barrier, inc=1, device_id=device(axis, by), device_id_type=MESH)
    pl.semaphore_wait(barrier, 9)

    counter = [I0]
    started = []

    def remote(src, dst, axis, by):
        i = counter[I0]
        counter[I0] += 1
        copy = pltpu.make_async_remote_copy(
            src_ref=src, dst_ref=dst, send_sem=send.at[i], recv_sem=recv.at[i], device_id=device(axis, by), device_id_type=MESH
        )
        copy.start()
        started.append(copy)
        return copy

    parts = []
    for n, (r0, rows, order) in enumerate(PARTS):
        p = Part()
        p.r0, p.rows, p.order = r0, rows, order
        p.h = (pl.ds(r0, H0), pl.ds(r0 + H0, rows - H0))
        b = bufs[n * PART_BUFS : (n + 1) * PART_BUFS]
        (p.own0, p.own1, p.ownr, p.ownl) = b[0:4]
        p.rec = (b[4:10], b[10:16], b[16:22])
        p.keep2 = b[22:26]
        p.keep3 = b[26:30]
        p.left = [at(a, -1) for a in order]
        p.right = [at(a, 1) for a in order]
        p.far = [at(a, 2) for a in order]
        p.me = [here[a] for a in order]
        p.second = 0 if order[I1] < order[I2] else 1
        parts.append(p)

    def source(p, piece, half):
        index = [slice(None)] * 3
        index[p.order[I0]] = piece
        return pk.at[(*index, p.h[half])]

    def pick(p, ref, j):
        return ref.at[j] if p.second == 0 else ref.at[:, j]

    for n, p in enumerate(parts):
        a = p.order[I0]
        far_l, far_r, dir_l, dir_r, com_l, com_r = p.rec[I0]
        p.c_far = (remote(source(p, p.far[I0], 0), far_l, a, 1), remote(source(p, p.far[I0], 1), far_r, a, -1))
    for n, p in enumerate(parts):
        a = p.order[I0]
        far_l, far_r, dir_l, dir_r, com_l, com_r = p.rec[I0]
        p.c_dir = (remote(source(p, p.right[I0], 1), dir_l, a, 1), remote(source(p, p.left[I0], 0), dir_r, a, -1))
        p.loads = [
            pltpu.make_async_copy(src, dst, local.at[4 * n + i])
            for i, (src, dst) in enumerate(
                (
                    (source(p, p.right[I0], 0), p.ownr),
                    (source(p, p.left[I0], 1), p.ownl),
                    (source(p, p.me[I0], 0), p.own0),
                    (source(p, p.me[I0], 1), p.own1),
                )
            )
        ]
        for load in p.loads:
            load.start()

    def each(count, body):
        lax.fori_loop(0, count, lambda i, _: (body(i), None)[I1], None)

    for p in parts:
        p.c_far[I0].wait_recv()
        p.c_far[I1].wait_recv()
        p.loads[I0].wait()
        p.loads[I1].wait()
    for p in parts:
        p.c_com = []
    for jj in range(4):
        for p in parts:
            j = (p.far, p.right, p.left, p.me)[jj][I1]
            pair = []
            for got, own, to, by in ((p.rec[I0][I0], p.ownr, p.rec[I0][I4], 1), (p.rec[I0][I1], p.ownl, p.rec[I0][I4 + 1], -1)):
                got, own, to = pick(p, got, j), pick(p, own, j), pick(p, to, j)

                def add(i, got=got, own=own):
                    own[i] = (own[i].astype(F32) + got[i].astype(F32)).astype(BF)

                each(4, add)
                pair.append(remote(own, to, p.order[I0], by))
            p.c_com.append(pair)
    for p in parts:
        p.c_dir[I0].wait_recv()
        p.c_dir[I1].wait_recv()
        p.loads[I2].wait()
        p.loads[I3].wait()

    for jj in range(4):
        for p in parts:
            a = p.order[I1]
            j = (p.far, p.right, p.left, p.me)[jj][I1]
            p.c_com[jj][I0].wait_recv()
            p.c_com[jj][I1].wait_recv()
            _, _, dir_l, dir_r, com_l, com_r = p.rec[I0]
            far2_l, far2_r, dir2_l, dir2_r, _, _ = p.rec[I1]
            keep0 = {1: p.keep2[I0], 3: p.keep2[I2]}.get(jj)
            keep1 = {2: p.keep2[I1], 3: p.keep2[I3]}.get(jj)
            for own, d, c, keep in ((p.own0, dir_r, com_l, keep0), (p.own1, dir_l, com_r, keep1)):
                own, d, c = pick(p, own, j), pick(p, d, j), pick(p, c, j)

                def add(i, own=own, d=d, c=c, keep=keep):
                    total = own[i].astype(F32) + d[i].astype(F32) + c[i].astype(F32)
                    if keep is None:
                        own[i] = total.astype(BF)
                    else:
                        keep[i] = total

                each(4, add)
            if jj == 0:
                p.c_far = (remote(pick(p, p.own0, j), far2_l, a, 1), remote(pick(p, p.own1, j), far2_r, a, -1))
            elif jj == 1:
                p.c_dir = [remote(pick(p, p.own1, j), dir2_l, a, 1)]
            elif jj == 2:
                p.c_dir.append(remote(pick(p, p.own0, j), dir2_r, a, -1))

    for p in parts:
        p.c_far[I0].wait_recv()
        p.c_far[I1].wait_recv()
        p.c_com = []
    for kk in range(4):
        for p in parts:
            k = (p.far, p.right, p.left, p.me)[kk][I2]
            pair = []
            for got, keep, to, by in ((p.rec[I1][I0], p.keep2[I0], p.rec[I1][I4], 1), (p.rec[I1][I1], p.keep2[I1], p.rec[I1][5], -1)):
                got[k] = (keep[k] + got[k].astype(F32)).astype(BF)
                pair.append(remote(got.at[k], to.at[k], p.order[I1], by))
            p.c_com.append(pair)
    for p in parts:
        p.c_dir[I0].wait_recv()
        p.c_dir[I1].wait_recv()

    for kk in range(4):
        for p in parts:
            a = p.order[I2]
            k = (p.far, p.right, p.left, p.me)[kk][I2]
            p.c_com[kk][I0].wait_recv()
            p.c_com[kk][I1].wait_recv()
            _, _, dir_l, dir_r, com_l, com_r = p.rec[I1]
            far3_l, far3_r, dir3_l, dir3_r, _, _ = p.rec[I2]
            keep0 = {1: p.keep3[I0], 3: p.keep3[I2]}.get(kk)
            keep1 = {2: p.keep3[I1], 3: p.keep3[I3]}.get(kk)
            total0 = p.keep2[I2][k] + dir_r[k].astype(F32) + com_l[k].astype(F32)
            total1 = p.keep2[I3][k] + dir_l[k].astype(F32) + com_r[k].astype(F32)
            if keep0 is None:
                dir_r[k] = total0.astype(BF)
            else:
                keep0[...] = total0
            if keep1 is None:
                dir_l[k] = total1.astype(BF)
            else:
                keep1[...] = total1
            if kk == 0:
                p.c_far = (remote(dir_r.at[k], far3_l, a, 1), remote(dir_l.at[k], far3_r, a, -1))
            elif kk == 1:
                p.c_dir = [remote(dir_l.at[k], dir3_l, a, 1)]
            elif kk == 2:
                p.c_dir.append(remote(dir_r.at[k], dir3_r, a, -1))

    for p in parts:
        p.c_com = []
        for got, keep, to, by, c in (
            (p.rec[I2][I0], p.keep3[I0], p.rec[I2][I4], 1, p.c_far[I0]),
            (p.rec[I2][I1], p.keep3[I1], p.rec[I2][5], -1, p.c_far[I1]),
        ):
            c.wait_recv()
            got[...] = (keep[...] + got[...].astype(F32)).astype(BF)
            p.c_com.append(remote(got, to, p.order[I2], by))
    squares = jnp.zeros((8, 128), F32)
    for p in parts:
        for c in (*p.c_dir, *p.c_com):
            c.wait_recv()
        _, _, dir_l, dir_r, com_l, com_r = p.rec[I2]
        for keep, d, c, rows in ((p.keep3[I2], dir_r, com_l, p.h[I0]), (p.keep3[I3], dir_l, com_r, p.h[I1])):
            g = (keep[...] + d[...].astype(F32) + c[...].astype(F32)).astype(BF).astype(F32)
            gs[rows, :] = g
            squares += jnp.sum((g * g).reshape(-1, 8, 128), axis=0)

    for axis in range(3):
        sq[axis] = squares
        copies = [remote(sq.at[axis], sqr.at[axis, by - 1], axis, by) for by in (1, 2, 3)]
        for i, c in enumerate(copies):
            c.wait_recv()
            squares += sqr[axis, i]
    total = jnp.sum(squares, axis=(0, 1), keepdims=True)
    factor = jnp.minimum(1.0, 0.5 * lax.rsqrt(total / COUNT + 1e-30))

    z = here[I2]
    block = 80

    def adamw(i):
        rows = pl.ds(pl.multiple_of(i * block, block), block)
        g = gs[rows, :] * factor
        w = wo[z, rows, :].astype(F32)
        new_m = 0.9 * m[rows, :] + 0.1 * g
        new_v = 0.95 * v[rows, :] + 0.05 * g * g
        mo[rows, :] = new_m
        vo[rows, :] = new_v
        wn[rows, :] = (w - 0.02 * (new_m * lax.rsqrt(new_v + 1e-8) + 0.1 * w)).astype(BF)

    each(ROWS // block, adamw)

    keep_copy = pltpu.make_async_copy(wn, wg.at[here[I0], here[I1], here[I2]], one_sem)
    keep_copy.start()

    def place(p, i, j, k, half):
        index = [None] * 3
        for a, value in zip(p.order, (i, j, k)):
            index[a] = slice(None) if value is None else value
        return wg.at[(*index, p.h[half])]

    def spread(p, axis, i, j, k, src=None):
        ref = [src[h] if src else place(p, i, j, k, h) for h in range(2)]
        to = [place(p, i, j, k, h) for h in range(2)]
        a = remote(ref[I0], to[I0], axis, 1)
        b = remote(ref[I1], to[I1], axis, -1)
        c = remote(ref[I1], to[I1], axis, 1)
        d = remote(ref[I0], to[I0], axis, -1)
        return a, b, c, d

    def forward(p, axis, copies, where_left, where_right):
        copies[I0].wait_recv()
        a = remote(place(p, *where_left, 0), place(p, *where_left, 0), axis, 1)
        copies[I1].wait_recv()
        b = remote(place(p, *where_right, 1), place(p, *where_right, 1), axis, -1)
        return a, b

    for p in parts:
        src = (wn.at[p.h[I0]], wn.at[p.h[I1]])
        i, j, k = p.me
        p.s3 = spread(p, p.order[I2], i, j, k, src)
        p.s2 = {}
    for p in parts:
        i, j, k = p.me
        p.s2[I0] = spread(p, p.order[I1], i, j, k, (wn.at[p.h[I0]], wn.at[p.h[I1]]))
    for p in parts:
        i, j, k = p.me
        p.f3 = forward(p, p.order[I2], p.s3, (i, j, p.left[I2]), (i, j, p.right[I2]))
    for p in parts:
        i, j, k = p.me
        p.s3[I2].wait_recv()
        p.s3[I3].wait_recv()
        p.s2[I1] = spread(p, p.order[I1], i, j, p.left[I2])
        p.s2[I2] = spread(p, p.order[I1], i, j, p.right[I2])
    keep_copy.wait()
    for p in parts:
        i, j, k = p.me
        p.f3[I0].wait_recv()
        p.f3[I1].wait_recv()
        p.s2[I3] = spread(p, p.order[I1], i, j, p.far[I2])
        p.f2 = {}
        p.s1, p.f1 = {}, {}
    for p in parts:
        i, j, k = p.me
        p.s1[I0] = spread(p, p.order[I0], i, j, None)
    for kk in range(4):
        for p in parts:
            i, j, _ = p.me
            k = (p.me, p.left, p.right, p.far)[kk][I2]
            p.f2[kk] = forward(p, p.order[I1], p.s2[kk], (i, p.left[I1], k), (i, p.right[I1], k))
    for p in parts:
        for kk in range(4):
            p.s2[kk][I2].wait_recv()
            p.s2[kk][I3].wait_recv()
        i, j, _ = p.me
        p.s1[I1] = spread(p, p.order[I0], i, p.left[I1], None)
        p.s1[I2] = spread(p, p.order[I0], i, p.right[I1], None)
    for p in parts:
        for kk in range(4):
            p.f2[kk][I0].wait_recv()
            p.f2[kk][I1].wait_recv()
        i, j, _ = p.me
        p.s1[I3] = spread(p, p.order[I0], i, p.far[I1], None)
    for jj in range(4):
        for p in parts:
            j = (p.me, p.left, p.right, p.far)[jj][I1]
            p.f1[jj] = forward(p, p.order[I0], p.s1[jj], (p.left[I0], j, None), (p.right[I0], j, None))
    for p in parts:
        for jj in range(4):
            for c in (*p.s1[jj][2:], *p.f1[jj]):
                c.wait_recv()
    for c in started:
        c.wait_send()


PART_BUFS = 30
COPIES = 3 * 30 + 9 + 3 * (6 + 24 + 24)


def step(pk, wo, m, v):
    bufs = []
    for r0, rows, order in PARTS:
        h = (H0, rows - H0)
        big = lambda half, t=BF: pltpu.VMEM((4, 4, h[half], 128), t)
        mid = lambda half, t=BF: pltpu.VMEM((4, h[half], 128), t)
        low = lambda half, t=BF: pltpu.VMEM((h[half], 128), t)
        bufs += [big(0), big(1), big(0), big(1)]
        for kind in (big, mid, low):
            bufs += [kind(0), kind(1), kind(1), kind(0), kind(0), kind(1)]
        for kind in (mid, low):
            bufs += [kind(0, F32), kind(1, F32), kind(0, F32), kind(1, F32)]
    return pl.pallas_call(
        step_kernel,
        out_shape=[
            jax.ShapeDtypeStruct((4, 4, 4, ROWS, 128), BF),
            jax.ShapeDtypeStruct((ROWS, 128), F32),
            jax.ShapeDtypeStruct((ROWS, 128), F32),
        ],
        in_specs=[ANY, VM, VM, VM],
        out_specs=[ANY, VM, VM],
        scratch_shapes=[
            pltpu.VMEM((ROWS, 128), BF),
            pltpu.VMEM((ROWS, 128), F32),
            pltpu.VMEM((3, 8, 128), F32),
            pltpu.VMEM((3, 3, 8, 128), F32),
            *bufs,
            pltpu.SemaphoreType.DMA((COPIES,)),
            pltpu.SemaphoreType.DMA((COPIES,)),
            pltpu.SemaphoreType.DMA((12,)),
            pltpu.SemaphoreType.DMA,
        ],
        compiler_params=pltpu.CompilerParams(collective_id=0, has_side_effects=True, vmem_limit_bytes=60 * 1024 * 1024),
        name="step",
    )(pk, wo, m, v)


def flat_of(x):
    layers, rows, columns = x.shape
    x = x.transpose(1, 0, 2).reshape(rows, layers, columns // 128, 128).transpose(0, 2, 1, 3)
    return x.reshape(500, 128)


def flat_to(x, shape):
    layers, rows, columns = shape
    x = x.reshape(rows, columns // 128, layers, 128).transpose(0, 2, 1, 3).reshape(rows, layers, columns)
    return x.transpose(1, 0, 2)


def solution(mesh):
    def run(*arrays):
        terms, weights, m, v = (arrays[i : i + 3] for i in (0, 3, 6, 9))
        pg, pd = perm_gu(), perm_dn()
        c = lambda a: jnp.asarray(a, BF)
        packed = pack(c(pg), c(pd), *[t[0] for t in terms])
        line = lax.div(lax.axis_index("dp"), 4)
        lines = [lax.dynamic_slice_in_dim(w, line * n, n, 1) for w, n in zip(weights, (40, 40, 200))]
        own = pack(c(pg), c(pd), *lines)[0]
        pm, pv = moments_in([flat_of(x) for x in (*m, *v)])
        wg, mo, vo = step(packed.reshape(4, 4, 4, ROWS, 128), own, pm, pv)
        outs = unpack(c(pg.T), c(pd.T), wg.reshape(16, 4, ROWS, 128), mo, vo)
        return (*outs[:3], *[flat_to(x, one.shape) for x, one in zip(outs[3:], (*m, *v))])

    all_of, cut = P(None, None, None), P(None, "dp", None)
    return jax.shard_map(
        run,
        mesh=mesh,
        in_specs=(P(("rep", "dp"), None, None, None),) * 3 + (all_of,) * 3 + (cut,) * 6,
        out_specs=(P("rep", None, None),) * 3 + (P("rep", "dp", None),) * 6,
        check_vma=False,
    )
```

```python
import jax
import jax.numpy as jnp
import numpy as np
from jax import lax
from jax.experimental import pallas as pl
from jax.experimental.pallas import tpu as pltpu
from jax.sharding import PartitionSpec as P

MESH = pl.DeviceIdType.MESH
BF, F32 = jnp.bfloat16, jnp.float32
ANY = pl.BlockSpec(memory_space=pl.ANY)
VM = pl.BlockSpec(memory_space=pltpu.VMEM)
LANES = 128
X, Y, Z = range(3)
FIRST, SECOND, THIRD = range(3)
LEFT, RIGHT, FAR, ME = -1, 1, 2, 0
LAYERS = (0, 1)
COUNT = 3 * 2 * 640 * 3200

ROWS = 504
HALF = (256, 248)
SPAN = (pl.ds(0, 256), pl.ds(256, 248))
QUAD, PAIR, TAIL = 80, 40, 24
TALL = 104
ORDERS = ((X, Y, Z), (Y, Z, X), (Z, X, Y))
PARTS = range(3)
MANY = 9
SIDE, RING, GRID = 4, range(4), (4, 4, 4)


def perms():
    wide, last = np.zeros((160, 160), np.float32), np.zeros((96, 80), np.float32)
    even, odd = np.zeros((416, 400), np.float32), np.zeros((416, 400), np.float32)
    for z in RING:
        for r in range(10):
            for s in RING:
                wide[z * PAIR + s * 10 + r, s * 40 + z * 10 + r] = 1
            for s in LAYERS:
                last[z * TAIL + s * 10 + r, s * 40 + z * 10 + r] = 1
        for r in range(50):
            for s in LAYERS:
                even[z * TALL + s * 50 + r, s * 200 + z * 50 + r] = 1
                odd[z * TALL + 4 + s * 50 + r, s * 200 + z * 50 + r] = 1
    return wide, last, even, odd


def wide_rows(tile, layer):
    group, within = divmod(tile, 4)
    return group * QUAD + within % 2 * PAIR + within // 2 * 20 + layer * 10


def tall_rows(tile, layer):
    return tile % 3 * 200 + tile // 3 * 100 + layer * 50


def dot(a, b):
    return jnp.dot(a, b.astype(BF), preferred_element_type=F32)


def stack(values, axis=0):
    return jnp.concatenate(values, axis=axis)


def put(out, z, first, value):
    cut = HALF[0]
    end = first + value.shape[0]
    value = value.astype(BF) if first >= cut or end <= cut else value
    if first >= cut:
        out[1][z, first - cut : end - cut, :] = value
    elif end <= cut:
        out[0][z, first:end, :] = value
    else:
        out[0][z, first:cut, :] = value[: cut - first].astype(BF)
        out[1][z, : end - cut, :] = value[cut - first :].astype(BF)


def get(ref, z, first, end):
    cut = HALF[0]
    low, high = first // 16 * 16, -(-end // 16) * 16
    if low >= cut:
        value = ref[1][z, low - cut : min(high, ROWS) - cut, :].astype(F32)
    elif high <= cut:
        value = ref[0][z, low:high, :].astype(F32)
    else:
        value = stack([ref[0][z, low:cut, :].astype(F32), ref[1][z, : min(high, ROWS) - cut, :].astype(F32)])
    return value[first - low : end - low]


def pack_wide(wide, last, src, out):
    for first in range(0, 3072, 4 * LANES):
        x = [src[s, :, pl.ds(first + two * 2 * LANES, 2 * LANES)].astype(F32) for two in LAYERS for s in LAYERS]
        y = dot(wide, stack(x))
        for z in RING:
            one = y[z * PAIR : (z + 1) * PAIR]
            put(out, z, first // (4 * LANES) * QUAD, stack([one[:, :LANES], one[:, LANES:]]))
    y = dot(last, stack([src[s, :, pl.ds(3072, LANES)].astype(F32) for s in LAYERS]))
    for z in RING:
        put(out, z, ROWS - TAIL, y[z * TAIL : (z + 1) * TAIL])


def unpack_wide(wide, last, block, write):
    for first in range(0, 3072, 4 * LANES):
        row = first // (4 * LANES) * QUAD
        got = [get(block, z, row, row + QUAD) for z in RING]
        x = stack([stack([one[:PAIR] for one in got]), stack([one[PAIR:] for one in got])], 1)
        y = dot(wide, x)
        for two in LAYERS:
            for s in LAYERS:
                at = (two * 2 + s) * 40
                write(s, pl.ds(first + two * 2 * LANES, 2 * LANES), y[at : at + 40])
    y = dot(last, stack([get(block, z, ROWS - TAIL, ROWS) for z in RING]))
    for s in LAYERS:
        write(s, pl.ds(3072, LANES), y[s * 40 : (s + 1) * 40])


def pack_tall(even, odd, src, out):
    def columns(a, b):
        return stack([src[s, :, a * LANES : b * LANES].astype(F32) for s in LAYERS])

    a, b = dot(even, columns(0, 3)), dot(odd, columns(3, 5))
    for z in RING:
        one, rows = [], slice(z * TALL, (z + 1) * TALL)
        for pair in range(3):
            u = a[rows, pair * LANES : (pair + 1) * LANES]
            if pair == 2:
                one.append(u)
            else:
                v = b[rows, pair * LANES : (pair + 1) * LANES]
                one += [u[:96], u[96:] + v[:8], v[8:]]
        put(out, z, 0, stack(one))


def unpack_tall(even, odd, block, write):
    for tile in range(5):
        first = tall_rows(tile, 0) - tile // 3 * 4
        x = stack([get(block, z, first, first + TALL) for z in RING])
        y = dot((even, odd)[tile // 3], x)
        for s in LAYERS:
            write(s, pl.ds(tile * LANES, LANES), y[s * 200 : (s + 1) * 200])


def each(count, body, start=0):
    lax.fori_loop(start, count, lambda i, _: (body(i), None)[1], None)


class Part:
    pass


class Place:
    def __init__(self, partners):
        self.rep, dp = lax.axis_index("rep"), lax.axis_index("dp")
        self.here = (lax.div(dp, 16), lax.rem(lax.div(dp, 4), 4), lax.rem(dp, 4))
        barrier = pltpu.get_barrier_semaphore()
        for axis in (X, Y, Z):
            for by in partners:
                pl.semaphore_signal(barrier, inc=1, device_id=self.device(axis, by), device_id_type=MESH)
        pl.semaphore_wait(barrier, 3 * len(partners))
        self.count = 0
        self.started = []

    def at(self, axis, by):
        return lax.rem(self.here[axis] + (by + 4), 4)

    def device(self, axis, by):
        c = [self.at(a, by if a == axis else ME) for a in (X, Y, Z)]
        return (self.rep, c[X] * 16 + c[Y] * 4 + c[Z])

    def copy(self, src, dst, axis, by, send, recv):
        return pltpu.make_async_remote_copy(
            src_ref=src, dst_ref=dst, send_sem=send, recv_sem=recv, device_id=self.device(axis, by), device_id_type=MESH
        )

    def send(self, src, dst, axis, by, sems):
        copy = self.copy(src, dst, axis, by, sems[0].at[self.count], sems[1].at[self.count])
        self.count += 1
        copy.start()
        self.started.append(copy)
        return copy

    def parts(self):
        made = []
        for n in PARTS:
            p = Part()
            p.n, p.order = n, ORDERS[n]
            p.second = ORDERS[n][SECOND] < ORDERS[n][THIRD]
            made.append(p)
        return made

    def index(self, p, i, j, k):
        index = [None] * 3
        for a, value in zip(p.order, (i, j, k)):
            index[a] = slice(None) if value is None else value
        return tuple(index)


def step_kernel(*refs):
    grads, weights, m_in, v_in, mats = (refs[i:j] for i, j in ((0, 3), (3, 6), (6, 9), (9, 12), (12, 16)))
    new0, new1, mo, vo = refs[16:20]
    scratch = refs[20:]
    lines, scratch = scratch[:3], scratch[3:]
    own, scratch = [scratch[2 * n : 2 * n + 2] for n in PARTS], scratch[6:]
    packed, scratch = [scratch[2 * n : 2 * n + 2] for n in PARTS], scratch[6:]
    rec, scratch = [[scratch[18 * n + 6 * f : 18 * n + 6 * f + 6] for f in PARTS] for n in PARTS], scratch[54:]
    gs, sq, sqr, send, recv, early_send, early_recv, load_sem = scratch
    sems = (send, recv)

    place = Place((RIGHT, FAR, LEFT))
    at = place.at
    parts = place.parts()
    mats = [one[...] for one in mats]

    def line_copies(srcs, line, slot):
        for n, (src, height) in enumerate(zip(srcs, (40, 40, 200))):
            rows = pl.ds(pl.multiple_of(line * height, 8), height)
            yield pltpu.make_async_copy(src.at[:, rows, :], lines[n].at[slot], load_sem.at[slot, n])

    def pack(slot, outs):
        for n in PARTS:
            src = lines[n].at[slot]
            if n < 2:
                pack_wide(*mats[:2], src, outs[n])
            else:
                pack_tall(*mats[2:], src, outs[n])

    def distance(u):
        return lax.rem(6 - u + 3 * lax.div(u, 2) - 2 * lax.div(u, 3), 4)

    def where(t):
        u, w = lax.div(t, 4), lax.rem(t, 4)
        return w, lax.rem(u + w, 4)

    def line_of(t):
        a, b = where(t)
        return at(X, distance(a)), at(Y, distance(b))

    def start_line(t):
        x, y = line_of(t)
        for c in line_copies(grads, x * 4 + y, lax.rem(t, 2)):
            c.start()

    start_line(0)
    start_line(1)

    def first_copies(p, got, kind, piece, block):
        far_l, far_r, dir_l, dir_r = rec[p.n][FIRST][:4]
        axis = p.order[FIRST]
        todo = (
            ((0, far_l, RIGHT, 0), (1, far_r, LEFT, 1)),
            ((1, dir_l, RIGHT, 2),),
            ((0, dir_r, LEFT, 3),),
        )[kind]
        for half, to, by, s in todo:
            place.copy(got[half].at[piece], to.at[block], axis, by, early_send.at[p.n, s], early_recv.at[p.n, s]).start()

    def one_line(t):
        slot = lax.rem(t, 2)
        a, b = where(t)
        x, y = line_of(t)
        for c in line_copies(grads, x * 4 + y, slot):
            c.wait()
        pack(slot, [[half.at[x, y] for half in packed[n]] for n in PARTS])

        @pl.when(t < 14)
        def _():
            start_line(t + 2)

        for kind in range(3):

            @pl.when(a == kind)
            def _():
                first_copies(parts[0], packed[0], kind, (x, y), y)

            @pl.when(b == kind)
            def _():
                first_copies(parts[1], packed[1], kind, (x, y), x)

            first_copies(parts[2], packed[2], kind, (x, y, at(Z, (FAR, RIGHT, LEFT)[kind])), (x, y))

    each(16, one_line)

    for c in line_copies(weights, at(X, ME) * 4 + at(Y, ME), 0):
        c.start()
    for new, old in ((mo, m_in), (vo, v_in)):
        new[:, 480:ROWS, :] = jnp.zeros((3, TAIL, LANES), F32)
        for n in PARTS:
            rows, height, tiles = (tall_rows, 50, 5) if n == 2 else (wide_rows, 10, 25)
            for tile in range(tiles):
                for s in LAYERS:
                    new[n, pl.ds(rows(tile, s), height), :] = old[n][:, s, tile * LANES : (tile + 1) * LANES]
    for c in line_copies(weights, at(X, ME) * 4 + at(Y, ME), 0):
        c.wait()
    pack(0, own)

    def early_wait(p, s):
        ref = rec[p.n][FIRST][s]
        place.copy(ref, ref, p.order[FIRST], LEFT, early_send.at[p.n, s], early_recv.at[p.n, s]).wait_recv()

    def block(p, ref, j, k):
        return ref.at[(j, k) if p.second else (k, j)]

    def whole(p, ref, j):
        return ref.at[j] if p.second else ref.at[:, j]

    def total(refs):
        value = refs[0][...].astype(F32)
        for ref in refs[1:]:
            value = value + ref[...].astype(F32)
        return value

    def terms1(p, half, piece, j, k):
        return [packed[p.n][half].at[place.index(p, piece, j, k)]]

    def terms2(p, half, j, k):
        _, _, dir_l, dir_r, com_l, com_r = rec[p.n][FIRST]
        more = ((dir_r, com_l), (dir_l, com_r))[half]
        return terms1(p, half, p.me[FIRST], j, k) + [block(p, ref, j, k) for ref in more]

    def terms3(p, half, k):
        _, _, dir_l, dir_r, com_l, com_r = rec[p.n][SECOND]
        more = ((dir_r, com_l), (dir_l, com_r))[half]
        return terms2(p, half, p.me[SECOND], k) + [ref.at[k] for ref in more]

    STEPS = (FAR, RIGHT, LEFT, ME)
    LEAVES = {
        FAR: ((0, 3, 0, RIGHT), (1, 2, 1, LEFT)),
        RIGHT: ((1, 2, 2, RIGHT),),
        LEFT: ((0, 3, 3, LEFT),),
        ME: (),
    }
    COMBINE = ((0, 0, 4, RIGHT), (1, 1, 5, LEFT))

    for p in parts:
        p.me = [at(a, ME) for a in p.order]
        p.to = {by: [at(a, by) for a in p.order] for by in STEPS}
        early_wait(p, 0)
        early_wait(p, 1)
        p.com = {}
    for by in STEPS:
        for p in parts:
            j = p.to[by][SECOND]
            p.com[by] = []
            for half, got, to, way in COMBINE:
                got, to = (rec[p.n][FIRST][i] for i in (got, to))

                def add(k):
                    ref = block(p, got, j, k)
                    ref[...] = total(terms1(p, half, p.to[way][FIRST], j, k) + [ref]).astype(BF)

                each(SIDE, add)
                p.com[by].append(place.send(whole(p, got, j), whole(p, to, j), p.order[FIRST], way, sems))
    for p in parts:
        early_wait(p, 2)
        early_wait(p, 3)
        p.next = {}

    for by in STEPS:
        for p in parts:
            j = p.to[by][SECOND]
            for c in p.com[by]:
                c.wait_recv()
            for half, slot, target, way in LEAVES[by]:
                ref = rec[p.n][FIRST][slot]

                def add(k):
                    block(p, ref, j, k)[...] = total(terms2(p, half, j, k)).astype(BF)

                each(SIDE, add)
                p.next[target] = place.send(whole(p, ref, j), rec[p.n][SECOND][target], p.order[SECOND], way, sems)

    for p in parts:
        p.next[0].wait_recv()
        p.next[1].wait_recv()
    for by in STEPS:
        for p in parts:
            k = p.to[by][THIRD]
            p.com[by] = []
            for half, got, to, way in COMBINE:
                got, to = (rec[p.n][SECOND][i].at[k] for i in (got, to))
                got[...] = total(terms2(p, half, p.to[way][SECOND], k) + [got]).astype(BF)
                p.com[by].append(place.send(got, to, p.order[SECOND], way, sems))
    for p in parts:
        p.next[2].wait_recv()
        p.next[3].wait_recv()
        p.next = {}

    for by in STEPS:
        for p in parts:
            k = p.to[by][THIRD]
            for c in p.com[by]:
                c.wait_recv()
            for half, slot, target, way in LEAVES[by]:
                ref = rec[p.n][SECOND][slot].at[k]
                ref[...] = total(terms3(p, half, k)).astype(BF)
                p.next[target] = place.send(ref, rec[p.n][THIRD][target], p.order[THIRD], way, sems)

    for p in parts:
        p.com = []
        for half, got, to, way in COMBINE:
            p.next[got].wait_recv()
            got, to = (rec[p.n][THIRD][i] for i in (got, to))
            got[...] = total(terms3(p, half, p.to[way][THIRD]) + [got]).astype(BF)
            p.com.append(place.send(got, to, p.order[THIRD], way, sems))
    squares = jnp.zeros((8, LANES), F32)
    for p in parts:
        for c in (p.next[2], p.next[3], *p.com):
            c.wait_recv()
        _, _, dir_l, dir_r, com_l, com_r = rec[p.n][THIRD]
        for half in LAYERS:
            g = total(terms3(p, half, p.me[THIRD]) + [(dir_r, dir_l)[half], (com_l, com_r)[half]]).astype(BF).astype(F32)
            gs[p.n, SPAN[half], :] = g
            squares += jnp.sum((g * g).reshape(-1, 8, LANES), axis=0)

    for axis in (X, Y, Z):
        sq[axis] = squares
        copies = [place.send(sq.at[axis], sqr.at[axis, i], axis, by, sems) for i, by in enumerate((RIGHT, FAR, LEFT))]
        for i, c in enumerate(copies):
            c.wait_recv()
            squares += sqr[axis, i]
    squares = jnp.sum(squares, axis=(0, 1), keepdims=True)
    factor = jnp.minimum(1.0, 0.5 * lax.rsqrt(squares / COUNT + 1e-30))

    for n in PARTS:
        for half in LAYERS:
            rows = SPAN[half]
            g = gs[n, rows, :] * factor
            w = own[n][half][at(Z, ME)].astype(F32)
            m = 0.9 * mo[n, rows, :] + 0.1 * g
            v = 0.95 * vo[n, rows, :] + 0.05 * g * g
            mo[n, rows, :] = m
            vo[n, rows, :] = v
            (new0, new1)[half][n] = (w - 0.02 * (m * lax.rsqrt(v + 1e-8) + 0.1 * w)).astype(BF)

    for c in place.started:
        c.wait_send()
    for p in parts:
        for s in RING:
            ref = rec[p.n][FIRST][s]
            place.copy(ref, ref, p.order[FIRST], LEFT, early_send.at[p.n, s], early_recv.at[p.n, s]).wait_send()


def halves(*lead, dtype=BF):
    return [pltpu.VMEM((*lead, h, LANES), dtype) for h in HALF]


def shape(*dims, dtype=BF):
    return jax.ShapeDtypeStruct(dims, dtype)


def step(grads, weights, m, v, mats):
    rec = []
    for lead in ((4, 4), (4,), ()):
        a, b = halves(*lead)
        rec += [a, b, b, a, a, b]
    copies = 87
    return pl.pallas_call(
        step_kernel,
        out_shape=[shape(3, HALF[0], LANES), shape(3, HALF[1], LANES)] + [shape(3, ROWS, LANES, dtype=F32)] * 2,
        in_specs=[ANY] * 6 + [VM] * 10,
        out_specs=[VM] * 4,
        scratch_shapes=[
            pltpu.VMEM((2, 2, 40, 3200), BF),
            pltpu.VMEM((2, 2, 40, 3200), BF),
            pltpu.VMEM((2, 2, 200, 640), BF),
            *halves(4) * 3,
            *halves(*GRID) * 3,
            *rec * 3,
            pltpu.VMEM((3, ROWS, LANES), F32),
            pltpu.VMEM((3, 8, LANES), F32),
            pltpu.VMEM((3, 3, 8, LANES), F32),
            pltpu.SemaphoreType.DMA((copies,)),
            pltpu.SemaphoreType.DMA((copies,)),
            pltpu.SemaphoreType.DMA((3, 4)),
            pltpu.SemaphoreType.DMA((3, 4)),
            pltpu.SemaphoreType.DMA((2, 3)),
        ],
        compiler_params=pltpu.CompilerParams(collective_id=0, has_side_effects=True, vmem_limit_bytes=67043328),
        name="step",
    )(*grads, *weights, *m, *v, *mats)


def gather_kernel(*refs):
    new, moments, mats, outs, moved = (refs[i:j] for i, j in ((0, 2), (2, 4), (4, 8), (8, 11), (11, 17)))
    scratch = refs[17:]
    got = [scratch[2 * n : 2 * n + 2] for n in PARTS]
    send, recv, late_send, late_recv = scratch[6:]
    sems = (send, recv)

    place = Place((RIGHT, LEFT))
    at = place.at
    parts = place.parts()
    for p in parts:
        p.me, p.left, p.right, p.far = ([at(a, by) for a in p.order] for by in (ME, LEFT, RIGHT, FAR))
        p.steps = (p.me, p.left, p.right, p.far)

    def ref_of(p, half, i, j, k):
        return got[p.n][half].at[place.index(p, i, j, k)]

    def spread(p, axis, i, j, k, mine=False):
        to = [ref_of(p, h, i, j, k) for h in LAYERS]
        src = [new[h].at[p.n] for h in LAYERS] if mine else to
        return [place.send(src[h], to[h], axis, by, sems) for h, by in ((0, RIGHT), (1, LEFT), (1, RIGHT), (0, LEFT))]

    def forward(p, axis, copies, from_left, from_right):
        copies[0].wait_recv()
        left = ref_of(p, 0, *from_left)
        a = place.send(left, left, axis, RIGHT, sems)
        copies[1].wait_recv()
        right = ref_of(p, 1, *from_right)
        return a, place.send(right, right, axis, LEFT, sems)

    def arrived(*copies):
        for c in copies:
            c.wait_recv()

    def chunk(p, axis_place, step):
        i, value = axis_place, step
        return (i, None, value) if p.n == 1 else (i, value, None)

    def late(p, jj, e, half, index, way):
        ref = ref_of(p, half, *index)
        return place.copy(ref, ref, p.order[FIRST], way, late_send.at[p.n, jj, e], late_recv.at[p.n, jj, e])

    def along(p):
        return p.order[THIRD if p.n == 1 else SECOND]

    def last_spread(p, jj, by):
        index = chunk(p, p.me[FIRST], at(along(p), by))
        for e, (h, way) in enumerate(((0, RIGHT), (1, LEFT), (1, RIGHT), (0, LEFT))):
            late(p, jj, e, h, index, way).start()

    for p in parts:
        p.s3 = spread(p, p.order[THIRD], *p.me, mine=True)
    for p in parts:
        p.s2, p.f2 = [spread(p, p.order[SECOND], *p.me, mine=True)], []
    for p in parts:
        for h in LAYERS:
            ref_of(p, h, *p.me)[...] = new[h][p.n]
    for p in parts:
        i, j, k = p.me
        p.f3 = forward(p, p.order[THIRD], p.s3, (i, j, p.left[THIRD]), (i, j, p.right[THIRD]))
    for p in parts:
        arrived(*p.s3[2:])
        for k in (p.left[THIRD], p.right[THIRD]):
            p.s2.append(spread(p, p.order[SECOND], *p.me[:THIRD], k))
    for p in parts:
        arrived(*p.f3)
        p.s2.append(spread(p, p.order[SECOND], *p.me[:THIRD], p.far[THIRD]))
        if p.n != 1:
            last_spread(p, 0, ME)
    for step, by in enumerate((ME, LEFT, RIGHT, FAR)):
        for p in parts:
            i, k = p.me[FIRST], p.steps[step][THIRD]
            p.f2.append(forward(p, p.order[SECOND], p.s2[step], (i, p.left[SECOND], k), (i, p.right[SECOND], k)))
        p = parts[1]
        if step:
            arrived(*p.s2[step - 1][2:], *p.f2[step - 1])
            last_spread(p, step - 1, (ME, LEFT, RIGHT)[step - 1])
    for p in parts:
        if p.n == 1:
            arrived(*p.s2[3][2:], *p.f2[3])
            last_spread(p, 3, FAR)
        else:
            for copies in p.s2:
                arrived(*copies[2:])
            last_spread(p, 1, LEFT)
            last_spread(p, 2, RIGHT)
            for copies in p.f2:
                arrived(*copies)
            last_spread(p, 3, FAR)

    for out, one in zip((moved[:3], moved[3:]), moments):
        for n in PARTS:
            rows, height, tiles = (tall_rows, 50, 5) if n == 2 else (wide_rows, 10, 25)
            for tile in range(tiles):
                for s in LAYERS:
                    out[n][:, s, tile * LANES : (tile + 1) * LANES] = one[n, pl.ds(rows(tile, s), height), :]

    mats = [one[...] for one in mats]

    def line(p, x, y):
        block = [half.at[x, y] for half in got[p.n]]
        height = 200 if p.n == 2 else 40
        rows = pl.ds(pl.multiple_of((x * 4 + y) * height, 8), height)

        def write(layer, columns, value):
            outs[p.n][layer, rows, columns] = value.astype(BF)

        if p.n == 2:
            unpack_tall(*mats[2:], block, write)
        else:
            unpack_wide(*mats[:2], block, write)

    def distance(jj):
        return 3 * lax.rem(jj, 2) + lax.div(jj, 2) - 2 * lax.div(jj, 3)

    def last(jj):
        @pl.when(jj < 4)
        def _():
            for p in parts:
                value = at(along(p), distance(jj))
                left, right = (chunk(p, i, value) for i in (p.left[FIRST], p.right[FIRST]))
                late(p, jj, 0, 0, left, LEFT).wait_recv()
                late(p, jj, 4, 0, left, RIGHT).start()
                late(p, jj, 1, 1, right, LEFT).wait_recv()
                late(p, jj, 5, 1, right, LEFT).start()
            for p in parts:
                value = at(along(p), distance(jj))
                left, right = (chunk(p, i, value) for i in (p.left[FIRST], p.right[FIRST]))
                late(p, jj, 2, 1, left, LEFT).wait_recv()
                late(p, jj, 3, 0, right, LEFT).wait_recv()

        before = jj - 1

        @pl.when(jj > 0)
        def _():
            for p in parts:
                far = chunk(p, p.far[FIRST], at(along(p), distance(before)))
                late(p, before, 4, 0, far, LEFT).wait_recv()
                late(p, before, 5, 1, far, LEFT).wait_recv()

        def one(i):
            which = jj - lax.div(i, 3)

            @pl.when((which >= 0) & (which < 4))
            def _():
                value = distance(which)
                line(parts[0], at(X, distance(i)), at(Y, value))
                line(parts[1], at(X, value), at(Y, distance(i)))

            @pl.when(jj > 0)
            def _():
                line(parts[2], at(X, distance(before)), i)

        each(SIDE, one)

    each(5, last)

    for c in place.started:
        c.wait_send()

    def drain(jj):
        for p in parts:
            index = chunk(p, p.me[FIRST], at(along(p), distance(jj)))
            for e, h in enumerate((0, 1, 1, 0, 0, 1)):
                late(p, jj, e, h, index, LEFT).wait_send()

    each(SIDE, drain)


def gather(new, moments, mats):
    copies = 90
    wide, tall = (10, 2, 3200), (50, 2, 640)
    outs = [pltpu.VMEM((2, 640, 3200), BF)] * 2 + [pltpu.VMEM((2, 3200, 640), BF)]
    outs += [pltpu.VMEM(one, F32) for one in (wide, wide, tall)] * 2
    return pl.pallas_call(
        gather_kernel,
        out_shape=outs,
        in_specs=[VM] * 8,
        out_specs=[VM] * MANY,
        scratch_shapes=[
            *halves(*GRID) * 3,
            pltpu.SemaphoreType.DMA((copies,)),
            pltpu.SemaphoreType.DMA((copies,)),
            pltpu.SemaphoreType.DMA((3, 4, 6)),
            pltpu.SemaphoreType.DMA((3, 4, 6)),
        ],
        compiler_params=pltpu.CompilerParams(collective_id=1, has_side_effects=True, vmem_limit_bytes=30 * 2**20),
        name="gather",
    )(*new, *moments, *mats)


def finish_kernel(*refs):
    held, outs, sem = refs[:MANY], refs[MANY : 2 * MANY], refs[2 * MANY]
    copies = [pltpu.make_async_copy(a, b, sem.at[n]) for n, (a, b) in enumerate(zip(held, outs))]
    for c in copies:
        c.start()
    for c in copies:
        c.wait()


def finish(held):
    return pl.pallas_call(
        finish_kernel,
        out_shape=[shape(*one.shape, dtype=one.dtype) for one in held],
        in_specs=[VM] * MANY,
        out_specs=[ANY] * MANY,
        scratch_shapes=[pltpu.SemaphoreType.DMA((MANY,))],
        compiler_params=pltpu.CompilerParams(vmem_limit_bytes=8 * 2**20),
        name="finish",
    )(*held)


def solution(mesh):
    def run(*arrays):
        terms, weights, m, v = (arrays[i : i + 3] for i in (0, 3, 6, 9))
        swap = lambda arrays: [x.transpose(1, 0, 2) for x in arrays]
        mats = perms()
        *new, mo, vo = step([t[0] for t in terms], weights, swap(m), swap(v), [jnp.asarray(a, BF) for a in mats])
        outs = finish(gather(new, (mo, vo), [jnp.asarray(a.T, BF) for a in mats]))
        return (*outs[:3], *swap(outs[3:]))

    all_of, cut = P(None, None, None), P(None, "dp", None)
    return jax.shard_map(
        run,
        mesh=mesh,
        in_specs=(P(("rep", "dp"), None, None, None),) * 3 + (all_of,) * 3 + (cut,) * 6,
        out_specs=(P("rep", None, None),) * 3 + (P("rep", "dp", None),) * 6,
        check_vma=False,
    )
```

```python
import jax
import jax.numpy as jnp
from jax import lax
from jax.experimental import pallas as pl
from jax.experimental.pallas import tpu as pltpu
from jax.sharding import PartitionSpec as P

MESH = pl.DeviceIdType.MESH
BF, F32 = jnp.bfloat16, jnp.float32
ANY = pl.BlockSpec(memory_space=pl.ANY)
VM = pl.BlockSpec(memory_space=pltpu.VMEM)
LANES = 128
X, Y, Z = range(3)
FIRST, SECOND, THIRD = range(3)
LEFT, RIGHT, FAR, ME = -1, 1, 2, 0
LAYERS = (0, 1)
COUNT = 3 * 2 * 640 * 3200

ROWS = 504
HALF = (256, 248)
SPAN = (pl.ds(0, 256), pl.ds(256, 248))
QUAD, TAIL = 80, 24
GROUPS = [range(t, min(t + 4, 25)) for t in range(0, 25, 4)]
ORDERS = ((X, Y, Z), (Y, Z, X), (Z, X, Y))
PARTS = range(3)
MANY = 9
SIDE, RING, GRID = 4, range(4), (4, 4, 4)


def wide_rows(tile, layer):
    return tile * 20 + layer * 10


def tall_rows(tile, layer):
    return tile * 100 + layer * 50


def stack(values, axis=0):
    return jnp.concatenate(values, axis=axis)


def put(out, z, first, value):
    cut = HALF[0]
    end = first + value.shape[0]
    value = value.astype(BF) if first >= cut or end <= cut else value
    if first >= cut:
        out[1][z, first - cut : end - cut, :] = value
    elif end <= cut:
        out[0][z, first:end, :] = value
    else:
        out[0][z, first:cut, :] = value[: cut - first].astype(BF)
        out[1][z, : end - cut, :] = value[cut - first :].astype(BF)


def get(ref, z, first, end):
    cut = HALF[0]
    low, high = first // 16 * 16, -(-end // 16) * 16
    if low >= cut:
        value = ref[1][z, low - cut : min(high, ROWS) - cut, :].astype(F32)
    elif high <= cut:
        value = ref[0][z, low:high, :].astype(F32)
    else:
        value = stack([ref[0][z, low:cut, :].astype(F32), ref[1][z, : min(high, ROWS) - cut, :].astype(F32)])
    return value[first - low : end - low]


def pack_wide(src, out):
    for group in range(7):
        tiles = GROUPS[group]
        x = [[src[s, :, pl.ds(t * LANES, LANES)].astype(F32) for s in LAYERS] for t in tiles]
        for z in RING:
            rows = [one[s][z * 10 : (z + 1) * 10] for one in x for s in LAYERS]
            if len(tiles) == 1:
                rows.append(jnp.zeros((SIDE, LANES), F32))
            put(out, z, group * QUAD, stack(rows))


def unpack_wide(block, write):
    for group in range(7):
        tiles = GROUPS[group]
        got = [get(block, z, group * QUAD, min(ROWS, (group + 1) * QUAD)) for z in RING]
        for n, t in enumerate(tiles):
            for s in LAYERS:
                row = n * 20 + s * 10
                write(s, pl.ds(t * LANES, LANES), stack([one[row : row + 10] for one in got]))


def pack_tall(src, out):
    x = [[src[s, :, pl.ds(t * LANES, LANES)].astype(F32) for s in LAYERS] for t in range(5)]
    for z in RING:
        rows = [one[s][z * 50 : (z + 1) * 50] for one in x for s in LAYERS]
        put(out, z, 0, stack([*rows, jnp.zeros((SIDE, LANES), F32)]))


def unpack_tall(block, write):
    got = [get(block, z, 0, ROWS) for z in RING]
    for t in range(5):
        for s in LAYERS:
            row = tall_rows(t, s)
            write(s, pl.ds(t * LANES, LANES), stack([one[row : row + 50] for one in got]))


def each(count, body, start=0):
    lax.fori_loop(start, count, lambda i, _: (body(i), None)[1], None)


class Part:
    pass


class Place:
    def __init__(self, partners):
        self.rep, dp = lax.axis_index("rep"), lax.axis_index("dp")
        self.here = (lax.div(dp, 16), lax.rem(lax.div(dp, 4), 4), lax.rem(dp, 4))
        barrier = pltpu.get_barrier_semaphore()
        for axis in (X, Y, Z):
            for by in partners:
                pl.semaphore_signal(barrier, inc=1, device_id=self.device(axis, by), device_id_type=MESH)
        pl.semaphore_wait(barrier, 3 * len(partners))
        self.count = 0
        self.started = []

    def at(self, axis, by):
        return lax.rem(self.here[axis] + (by + 4), 4)

    def device(self, axis, by):
        c = [self.at(a, by if a == axis else ME) for a in (X, Y, Z)]
        return (self.rep, c[X] * 16 + c[Y] * 4 + c[Z])

    def copy(self, src, dst, axis, by, send, recv):
        return pltpu.make_async_remote_copy(
            src_ref=src, dst_ref=dst, send_sem=send, recv_sem=recv, device_id=self.device(axis, by), device_id_type=MESH
        )

    def send(self, src, dst, axis, by, sems):
        copy = self.copy(src, dst, axis, by, sems[0].at[self.count], sems[1].at[self.count])
        self.count += 1
        copy.start()
        self.started.append(copy)
        return copy

    def parts(self):
        made = []
        for n in PARTS:
            p = Part()
            p.n, p.order = n, ORDERS[n]
            p.second = ORDERS[n][SECOND] < ORDERS[n][THIRD]
            made.append(p)
        return made

    def index(self, p, i, j, k):
        index = [None] * 3
        for a, value in zip(p.order, (i, j, k)):
            index[a] = slice(None) if value is None else value
        return tuple(index)


def step_kernel(*refs):
    grads, weights, m_in, v_in = (refs[i : i + 3] for i in (0, 3, 6, 9))
    new0, new1, mo, vo = refs[12:16]
    scratch = refs[16:]
    lines, scratch = scratch[:3], scratch[3:]
    own, scratch = [scratch[2 * n : 2 * n + 2] for n in PARTS], scratch[6:]
    packed, scratch = [scratch[2 * n : 2 * n + 2] for n in PARTS], scratch[6:]
    rec, scratch = [[scratch[18 * n + 6 * f : 18 * n + 6 * f + 6] for f in PARTS] for n in PARTS], scratch[54:]
    gs, sq, sqr, send, recv, early_send, early_recv, load_sem = scratch
    sems = (send, recv)

    place = Place((RIGHT, FAR, LEFT))
    at = place.at
    parts = place.parts()

    def line_copies(srcs, line, slot):
        for n, (src, height) in enumerate(zip(srcs, (40, 40, 200))):
            rows = pl.ds(pl.multiple_of(line * height, 8), height)
            yield pltpu.make_async_copy(src.at[:, rows, :], lines[n].at[slot], load_sem.at[slot, n])

    def pack(slot, outs):
        for n in PARTS:
            src = lines[n].at[slot]
            if n < 2:
                pack_wide(src, outs[n])
            else:
                pack_tall(src, outs[n])

    def distance(u):
        return lax.rem(6 - u + 3 * lax.div(u, 2) - 2 * lax.div(u, 3), 4)

    def where(t):
        u, w = lax.div(t, 4), lax.rem(t, 4)
        return w, lax.rem(u + w, 4)

    def line_of(t):
        a, b = where(t)
        return at(X, distance(a)), at(Y, distance(b))

    def start_line(t):
        x, y = line_of(t)
        for c in line_copies(grads, x * 4 + y, lax.rem(t, 2)):
            c.start()

    start_line(0)
    start_line(1)

    def first_copies(p, got, kind, piece, block):
        far_l, far_r, dir_l, dir_r = rec[p.n][FIRST][:4]
        axis = p.order[FIRST]
        todo = (
            ((0, far_l, RIGHT, 0), (1, far_r, LEFT, 1)),
            ((1, dir_l, RIGHT, 2),),
            ((0, dir_r, LEFT, 3),),
        )[kind]
        for half, to, by, s in todo:
            place.copy(got[half].at[piece], to.at[block], axis, by, early_send.at[p.n, s], early_recv.at[p.n, s]).start()

    def one_line(t):
        slot = lax.rem(t, 2)
        a, b = where(t)
        x, y = line_of(t)
        for c in line_copies(grads, x * 4 + y, slot):
            c.wait()
        pack(slot, [[half.at[x, y] for half in packed[n]] for n in PARTS])

        @pl.when(t < 14)
        def _():
            start_line(t + 2)

        for kind in range(3):

            @pl.when(a == kind)
            def _():
                first_copies(parts[0], packed[0], kind, (x, y), y)

            @pl.when(b == kind)
            def _():
                first_copies(parts[1], packed[1], kind, (x, y), x)

            first_copies(parts[2], packed[2], kind, (x, y, at(Z, (FAR, RIGHT, LEFT)[kind])), (x, y))

    each(16, one_line)

    for c in line_copies(weights, at(X, ME) * 4 + at(Y, ME), 0):
        c.start()
    for new, old in ((mo, m_in), (vo, v_in)):
        new[:, ROWS - TAIL : ROWS, :] = jnp.zeros((3, TAIL, LANES), F32)
        for n in PARTS:
            rows, height, tiles = (tall_rows, 50, 5) if n == 2 else (wide_rows, 10, 25)
            for tile in range(tiles):
                for s in LAYERS:
                    new[n, pl.ds(rows(tile, s), height), :] = old[n][:, s, tile * LANES : (tile + 1) * LANES]
    for c in line_copies(weights, at(X, ME) * 4 + at(Y, ME), 0):
        c.wait()
    pack(0, own)

    def early_wait(p, s):
        ref = rec[p.n][FIRST][s]
        place.copy(ref, ref, p.order[FIRST], LEFT, early_send.at[p.n, s], early_recv.at[p.n, s]).wait_recv()

    def block(p, ref, j, k):
        return ref.at[(j, k) if p.second else (k, j)]

    def whole(p, ref, j):
        return ref.at[j] if p.second else ref.at[:, j]

    def total(refs):
        value = refs[0][...].astype(F32)
        for ref in refs[1:]:
            value = value + ref[...].astype(F32)
        return value

    def terms1(p, half, piece, j, k):
        return [packed[p.n][half].at[place.index(p, piece, j, k)]]

    def terms2(p, half, j, k):
        _, _, dir_l, dir_r, com_l, com_r = rec[p.n][FIRST]
        more = ((dir_r, com_l), (dir_l, com_r))[half]
        return terms1(p, half, p.me[FIRST], j, k) + [block(p, ref, j, k) for ref in more]

    def terms3(p, half, k):
        _, _, dir_l, dir_r, com_l, com_r = rec[p.n][SECOND]
        more = ((dir_r, com_l), (dir_l, com_r))[half]
        return terms2(p, half, p.me[SECOND], k) + [ref.at[k] for ref in more]

    STEPS = (FAR, RIGHT, LEFT, ME)
    LEAVES = {
        FAR: ((0, 3, 0, RIGHT), (1, 2, 1, LEFT)),
        RIGHT: ((1, 2, 2, RIGHT),),
        LEFT: ((0, 3, 3, LEFT),),
        ME: (),
    }
    COMBINE = ((0, 0, 4, RIGHT), (1, 1, 5, LEFT))

    for p in parts:
        p.me = [at(a, ME) for a in p.order]
        p.to = {by: [at(a, by) for a in p.order] for by in STEPS}
        early_wait(p, 0)
        early_wait(p, 1)
        p.com = {}
    for by in STEPS:
        for p in parts:
            j = p.to[by][SECOND]
            p.com[by] = []
            for half, got, to, way in COMBINE:
                got, to = (rec[p.n][FIRST][i] for i in (got, to))

                def add(k):
                    ref = block(p, got, j, k)
                    ref[...] = total(terms1(p, half, p.to[way][FIRST], j, k) + [ref]).astype(BF)

                each(SIDE, add)
                p.com[by].append(place.send(whole(p, got, j), whole(p, to, j), p.order[FIRST], way, sems))
    for p in parts:
        early_wait(p, 2)
        early_wait(p, 3)
        p.next = {}

    for by in STEPS:
        for p in parts:
            j = p.to[by][SECOND]
            for c in p.com[by]:
                c.wait_recv()
            for half, slot, target, way in LEAVES[by]:
                ref = rec[p.n][FIRST][slot]

                def add(k):
                    block(p, ref, j, k)[...] = total(terms2(p, half, j, k)).astype(BF)

                each(SIDE, add)
                p.next[target] = place.send(whole(p, ref, j), rec[p.n][SECOND][target], p.order[SECOND], way, sems)

    for p in parts:
        p.next[0].wait_recv()
        p.next[1].wait_recv()
    for by in STEPS:
        for p in parts:
            k = p.to[by][THIRD]
            p.com[by] = []
            for half, got, to, way in COMBINE:
                got, to = (rec[p.n][SECOND][i].at[k] for i in (got, to))
                got[...] = total(terms2(p, half, p.to[way][SECOND], k) + [got]).astype(BF)
                p.com[by].append(place.send(got, to, p.order[SECOND], way, sems))
    for p in parts:
        p.next[2].wait_recv()
        p.next[3].wait_recv()
        p.next = {}

    for by in STEPS:
        for p in parts:
            k = p.to[by][THIRD]
            for c in p.com[by]:
                c.wait_recv()
            for half, slot, target, way in LEAVES[by]:
                ref = rec[p.n][SECOND][slot].at[k]
                ref[...] = total(terms3(p, half, k)).astype(BF)
                p.next[target] = place.send(ref, rec[p.n][THIRD][target], p.order[THIRD], way, sems)

    for p in parts:
        p.com = []
        for half, got, to, way in COMBINE:
            p.next[got].wait_recv()
            got, to = (rec[p.n][THIRD][i] for i in (got, to))
            got[...] = total(terms3(p, half, p.to[way][THIRD]) + [got]).astype(BF)
            p.com.append(place.send(got, to, p.order[THIRD], way, sems))
    squares = jnp.zeros((8, LANES), F32)
    for p in parts:
        for c in (p.next[2], p.next[3], *p.com):
            c.wait_recv()
        _, _, dir_l, dir_r, com_l, com_r = rec[p.n][THIRD]
        for half in LAYERS:
            g = total(terms3(p, half, p.me[THIRD]) + [(dir_r, dir_l)[half], (com_l, com_r)[half]]).astype(BF).astype(F32)
            gs[p.n, SPAN[half], :] = g
            squares += jnp.sum((g * g).reshape(-1, 8, LANES), axis=0)

    for axis in (X, Y, Z):
        sq[axis] = squares
        copies = [place.send(sq.at[axis], sqr.at[axis, i], axis, by, sems) for i, by in enumerate((RIGHT, FAR, LEFT))]
        for i, c in enumerate(copies):
            c.wait_recv()
            squares += sqr[axis, i]
    squares = jnp.sum(squares, axis=(0, 1), keepdims=True)
    factor = jnp.minimum(1.0, 0.5 * lax.rsqrt(squares / COUNT + 1e-30))

    for n in PARTS:
        for half in LAYERS:
            rows = SPAN[half]
            g = gs[n, rows, :] * factor
            w = own[n][half][at(Z, ME)].astype(F32)
            m = 0.9 * mo[n, rows, :] + 0.1 * g
            v = 0.95 * vo[n, rows, :] + 0.05 * g * g
            mo[n, rows, :] = m
            vo[n, rows, :] = v
            (new0, new1)[half][n] = (w - 0.02 * (m * lax.rsqrt(v + 1e-8) + 0.1 * w)).astype(BF)

    for c in place.started:
        c.wait_send()
    for p in parts:
        for s in RING:
            ref = rec[p.n][FIRST][s]
            place.copy(ref, ref, p.order[FIRST], LEFT, early_send.at[p.n, s], early_recv.at[p.n, s]).wait_send()


def halves(*lead, dtype=BF):
    return [pltpu.VMEM((*lead, h, LANES), dtype) for h in HALF]


def shape(*dims, dtype=BF):
    return jax.ShapeDtypeStruct(dims, dtype)


def step(grads, weights, m, v):
    rec = []
    for lead in ((4, 4), (4,), ()):
        a, b = halves(*lead)
        rec += [a, b, b, a, a, b]
    copies = 87
    return pl.pallas_call(
        step_kernel,
        out_shape=[shape(3, HALF[0], LANES), shape(3, HALF[1], LANES)] + [shape(3, ROWS, LANES, dtype=F32)] * 2,
        in_specs=[ANY] * 6 + [VM] * 6,
        out_specs=[VM] * 4,
        scratch_shapes=[
            pltpu.VMEM((2, 2, 40, 3200), BF),
            pltpu.VMEM((2, 2, 40, 3200), BF),
            pltpu.VMEM((2, 2, 200, 640), BF),
            *halves(4) * 3,
            *halves(*GRID) * 3,
            *rec * 3,
            pltpu.VMEM((3, ROWS, LANES), F32),
            pltpu.VMEM((3, 8, LANES), F32),
            pltpu.VMEM((3, 3, 8, LANES), F32),
            pltpu.SemaphoreType.DMA((copies,)),
            pltpu.SemaphoreType.DMA((copies,)),
            pltpu.SemaphoreType.DMA((3, 4)),
            pltpu.SemaphoreType.DMA((3, 4)),
            pltpu.SemaphoreType.DMA((2, 3)),
        ],
        compiler_params=pltpu.CompilerParams(collective_id=0, has_side_effects=True, vmem_limit_bytes=67043328),
        name="step",
    )(*grads, *weights, *m, *v)


def gather_kernel(*refs):
    new, moments, outs, moved = (refs[i:j] for i, j in ((0, 2), (2, 4), (4, 7), (7, 13)))
    scratch = refs[13:]
    got = [scratch[2 * n : 2 * n + 2] for n in PARTS]
    send, recv, late_send, late_recv = scratch[6:]
    sems = (send, recv)

    place = Place((RIGHT, LEFT))
    at = place.at
    parts = place.parts()
    for p in parts:
        p.me, p.left, p.right, p.far = ([at(a, by) for a in p.order] for by in (ME, LEFT, RIGHT, FAR))
        p.steps = (p.me, p.left, p.right, p.far)

    def ref_of(p, half, i, j, k):
        return got[p.n][half].at[place.index(p, i, j, k)]

    def spread(p, axis, i, j, k, mine=False):
        to = [ref_of(p, h, i, j, k) for h in LAYERS]
        src = [new[h].at[p.n] for h in LAYERS] if mine else to
        return [place.send(src[h], to[h], axis, by, sems) for h, by in ((0, RIGHT), (1, LEFT), (1, RIGHT), (0, LEFT))]

    def forward(p, axis, copies, from_left, from_right):
        copies[0].wait_recv()
        left = ref_of(p, 0, *from_left)
        a = place.send(left, left, axis, RIGHT, sems)
        copies[1].wait_recv()
        right = ref_of(p, 1, *from_right)
        return a, place.send(right, right, axis, LEFT, sems)

    def arrived(*copies):
        for c in copies:
            c.wait_recv()

    def chunk(p, axis_place, step):
        i, value = axis_place, step
        return (i, None, value) if p.n == 1 else (i, value, None)

    def late(p, jj, e, half, index, way):
        ref = ref_of(p, half, *index)
        return place.copy(ref, ref, p.order[FIRST], way, late_send.at[p.n, jj, e], late_recv.at[p.n, jj, e])

    def along(p):
        return p.order[THIRD if p.n == 1 else SECOND]

    def last_spread(p, jj, by):
        index = chunk(p, p.me[FIRST], at(along(p), by))
        for e, (h, way) in enumerate(((0, RIGHT), (1, LEFT), (1, RIGHT), (0, LEFT))):
            late(p, jj, e, h, index, way).start()

    for p in parts:
        p.s3 = spread(p, p.order[THIRD], *p.me, mine=True)
    for p in parts:
        p.s2, p.f2 = [spread(p, p.order[SECOND], *p.me, mine=True)], []
    for p in parts:
        for h in LAYERS:
            ref_of(p, h, *p.me)[...] = new[h][p.n]
    for p in parts:
        i, j, k = p.me
        p.f3 = forward(p, p.order[THIRD], p.s3, (i, j, p.left[THIRD]), (i, j, p.right[THIRD]))
    for p in parts:
        arrived(*p.s3[2:])
        for k in (p.left[THIRD], p.right[THIRD]):
            p.s2.append(spread(p, p.order[SECOND], *p.me[:THIRD], k))
    for p in parts:
        arrived(*p.f3)
        p.s2.append(spread(p, p.order[SECOND], *p.me[:THIRD], p.far[THIRD]))
        if p.n != 1:
            last_spread(p, 0, ME)
    for step, by in enumerate((ME, LEFT, RIGHT, FAR)):
        for p in parts:
            i, k = p.me[FIRST], p.steps[step][THIRD]
            p.f2.append(forward(p, p.order[SECOND], p.s2[step], (i, p.left[SECOND], k), (i, p.right[SECOND], k)))
        p = parts[1]
        if step:
            arrived(*p.s2[step - 1][2:], *p.f2[step - 1])
            last_spread(p, step - 1, (ME, LEFT, RIGHT)[step - 1])
    for p in parts:
        if p.n == 1:
            arrived(*p.s2[3][2:], *p.f2[3])
            last_spread(p, 3, FAR)
        else:
            for copies in p.s2:
                arrived(*copies[2:])
            last_spread(p, 1, LEFT)
            last_spread(p, 2, RIGHT)
            for copies in p.f2:
                arrived(*copies)
            last_spread(p, 3, FAR)

    for out, one in zip((moved[:3], moved[3:]), moments):
        for n in PARTS:
            rows, height, tiles = (tall_rows, 50, 5) if n == 2 else (wide_rows, 10, 25)
            for tile in range(tiles):
                for s in LAYERS:
                    out[n][:, s, tile * LANES : (tile + 1) * LANES] = one[n, pl.ds(rows(tile, s), height), :]


    def line(p, x, y):
        block = [half.at[x, y] for half in got[p.n]]
        height = 200 if p.n == 2 else 40
        rows = pl.ds(pl.multiple_of((x * 4 + y) * height, 8), height)

        def write(layer, columns, value):
            outs[p.n][layer, rows, columns] = value.astype(BF)

        if p.n == 2:
            unpack_tall(block, write)
        else:
            unpack_wide(block, write)

    def distance(jj):
        return 3 * lax.rem(jj, 2) + lax.div(jj, 2) - 2 * lax.div(jj, 3)

    def last(jj):
        @pl.when(jj < 4)
        def _():
            for p in parts:
                value = at(along(p), distance(jj))
                left, right = (chunk(p, i, value) for i in (p.left[FIRST], p.right[FIRST]))
                late(p, jj, 0, 0, left, LEFT).wait_recv()
                late(p, jj, 4, 0, left, RIGHT).start()
                late(p, jj, 1, 1, right, LEFT).wait_recv()
                late(p, jj, 5, 1, right, LEFT).start()
            for p in parts:
                value = at(along(p), distance(jj))
                left, right = (chunk(p, i, value) for i in (p.left[FIRST], p.right[FIRST]))
                late(p, jj, 2, 1, left, LEFT).wait_recv()
                late(p, jj, 3, 0, right, LEFT).wait_recv()

        before = jj - 1

        @pl.when(jj > 0)
        def _():
            for p in parts:
                far = chunk(p, p.far[FIRST], at(along(p), distance(before)))
                late(p, before, 4, 0, far, LEFT).wait_recv()
                late(p, before, 5, 1, far, LEFT).wait_recv()

        def one(i):
            which = jj - lax.div(i, 3)

            @pl.when((which >= 0) & (which < 4))
            def _():
                value = distance(which)
                line(parts[0], at(X, distance(i)), at(Y, value))
                line(parts[1], at(X, value), at(Y, distance(i)))

            @pl.when(jj > 0)
            def _():
                line(parts[2], at(X, distance(before)), i)

        each(SIDE, one)

    each(5, last)

    for c in place.started:
        c.wait_send()

    def drain(jj):
        for p in parts:
            index = chunk(p, p.me[FIRST], at(along(p), distance(jj)))
            for e, h in enumerate((0, 1, 1, 0, 0, 1)):
                late(p, jj, e, h, index, LEFT).wait_send()

    each(SIDE, drain)


def gather(new, moments):
    copies = 90
    wide, tall = (10, 2, 3200), (50, 2, 640)
    outs = [pltpu.VMEM((2, 640, 3200), BF)] * 2 + [pltpu.VMEM((2, 3200, 640), BF)]
    outs += [pltpu.VMEM(one, F32) for one in (wide, wide, tall)] * 2
    return pl.pallas_call(
        gather_kernel,
        out_shape=outs,
        in_specs=[VM] * 4,
        out_specs=[VM] * MANY,
        scratch_shapes=[
            *halves(*GRID) * 3,
            pltpu.SemaphoreType.DMA((copies,)),
            pltpu.SemaphoreType.DMA((copies,)),
            pltpu.SemaphoreType.DMA((3, 4, 6)),
            pltpu.SemaphoreType.DMA((3, 4, 6)),
        ],
        compiler_params=pltpu.CompilerParams(collective_id=1, has_side_effects=True, vmem_limit_bytes=30 * 2**20),
        name="gather",
    )(*new, *moments)


def finish_kernel(*refs):
    held, outs, sem = refs[:MANY], refs[MANY : 2 * MANY], refs[2 * MANY]
    copies = [pltpu.make_async_copy(a, b, sem.at[n]) for n, (a, b) in enumerate(zip(held, outs))]
    for c in copies:
        c.start()
    for c in copies:
        c.wait()


def finish(held):
    return pl.pallas_call(
        finish_kernel,
        out_shape=[shape(*one.shape, dtype=one.dtype) for one in held],
        in_specs=[VM] * MANY,
        out_specs=[ANY] * MANY,
        scratch_shapes=[pltpu.SemaphoreType.DMA((MANY,))],
        compiler_params=pltpu.CompilerParams(vmem_limit_bytes=8 * 2**20),
        name="finish",
    )(*held)


def solution(mesh):
    def run(*arrays):
        terms, weights, m, v = (arrays[i : i + 3] for i in (0, 3, 6, 9))
        swap = lambda arrays: [x.transpose(1, 0, 2) for x in arrays]
        *new, mo, vo = step([t[0] for t in terms], weights, swap(m), swap(v))
        outs = finish(gather(new, (mo, vo)))
        return (*outs[:3], *swap(outs[3:]))

    all_of, cut = P(None, None, None), P(None, "dp", None)
    return jax.shard_map(
        run,
        mesh=mesh,
        in_specs=(P(("rep", "dp"), None, None, None),) * 3 + (all_of,) * 3 + (cut,) * 6,
        out_specs=(P("rep", None, None),) * 3 + (P("rep", "dp", None),) * 6,
        check_vma=False,
    )
```

```python
import jax
import jax.numpy as jnp
from jax import lax
from jax.experimental import pallas as pl
from jax.experimental.pallas import tpu as pltpu
from jax.sharding import PartitionSpec as P

MESH = pl.DeviceIdType.MESH
BF, F32 = jnp.bfloat16, jnp.float32
ANY = pl.BlockSpec(memory_space=pl.ANY)
VM = pl.BlockSpec(memory_space=pltpu.VMEM)
LANES = 128
X, Y, Z = range(3)
FIRST, SECOND, THIRD = range(3)
LEFT, RIGHT, FAR, ME = -1, 1, 2, 0
LAYERS = (0, 1)
COUNT = 3 * 2 * 640 * 3200

ROWS = 504
HALF = (256, 248)
SPAN = (pl.ds(0, 256), pl.ds(256, 248))
QUAD, TAIL = 80, 24
GROUPS = [range(t, min(t + 4, 25)) for t in range(0, 25, 4)]
ORDERS = ((X, Y, Z), (Y, Z, X), (Z, X, Y))
PARTS = range(3)
MANY = 9
LAG = 2
ORDER = (ME, LEFT, RIGHT, FAR)
SIDE, RING, GRID = 4, range(4), (4, 4, 4)


def wide_rows(tile, layer):
    return tile * 20 + layer * 10


def tall_rows(tile, layer):
    return tile * 100 + layer * 50


def stack(values, axis=0):
    return jnp.concatenate(values, axis=axis)


def put(out, z, first, value):
    cut = HALF[0]
    end = first + value.shape[0]
    value = value.astype(BF) if first >= cut or end <= cut else value
    if first >= cut:
        out[1][z, first - cut : end - cut, :] = value
    elif end <= cut:
        out[0][z, first:end, :] = value
    else:
        out[0][z, first:cut, :] = value[: cut - first].astype(BF)
        out[1][z, : end - cut, :] = value[cut - first :].astype(BF)


def get(ref, z, first, end):
    cut = HALF[0]
    low, high = first // 16 * 16, -(-end // 16) * 16
    if low >= cut:
        value = ref[1][z, low - cut : min(high, ROWS) - cut, :].astype(F32)
    elif high <= cut:
        value = ref[0][z, low:high, :].astype(F32)
    else:
        value = stack([ref[0][z, low:cut, :].astype(F32), ref[1][z, : min(high, ROWS) - cut, :].astype(F32)])
    return value[first - low : end - low]


def pack_wide(src, out):
    for group in range(7):
        tiles = GROUPS[group]
        x = [[src[s, :, pl.ds(t * LANES, LANES)].astype(F32) for s in LAYERS] for t in tiles]
        for z in RING:
            rows = [one[s][z * 10 : (z + 1) * 10] for one in x for s in LAYERS]
            if len(tiles) == 1:
                rows.append(jnp.zeros((SIDE, LANES), F32))
            put(out, z, group * QUAD, stack(rows))


def unpack_wide(block, write):
    for group in range(7):
        tiles = GROUPS[group]
        got = [get(block, z, group * QUAD, min(ROWS, (group + 1) * QUAD)) for z in RING]
        for n, t in enumerate(tiles):
            for s in LAYERS:
                row = n * 20 + s * 10
                write(s, pl.ds(t * LANES, LANES), stack([one[row : row + 10] for one in got]))


def pack_tall(src, out):
    x = [[src[s, :, pl.ds(t * LANES, LANES)].astype(F32) for s in LAYERS] for t in range(5)]
    for z in RING:
        rows = [one[s][z * 50 : (z + 1) * 50] for one in x for s in LAYERS]
        put(out, z, 0, stack([*rows, jnp.zeros((SIDE, LANES), F32)]))


def unpack_tall(block, write):
    got = [get(block, z, 0, ROWS) for z in RING]
    for t in range(5):
        for s in LAYERS:
            row = tall_rows(t, s)
            write(s, pl.ds(t * LANES, LANES), stack([one[row : row + 50] for one in got]))


def each(count, body, start=0):
    lax.fori_loop(start, count, lambda i, _: (body(i), None)[1], None)


class Part:
    pass


class Place:
    def __init__(self, partners, other_core=False):
        self.rep, dp = lax.axis_index("rep"), lax.axis_index("dp")
        self.here = (lax.div(dp, 16), lax.rem(lax.div(dp, 4), 4), lax.rem(dp, 4))
        barrier = pltpu.get_barrier_semaphore()
        for axis in (X, Y, Z):
            for by in partners:
                pl.semaphore_signal(barrier, inc=1, device_id=self.device(axis, by), device_id_type=MESH)
        if other_core:
            pl.semaphore_signal(barrier, inc=1, device_id=self.other_core(), device_id_type=MESH)
        pl.semaphore_wait(barrier, 3 * len(partners) + other_core)
        self.count = 0
        self.started = []

    def at(self, axis, by):
        return lax.rem(self.here[axis] + (by + 4), 4)

    def device(self, axis, by):
        c = [self.at(a, by if a == axis else ME) for a in (X, Y, Z)]
        return (self.rep, c[X] * 16 + c[Y] * 4 + c[Z])

    def other_core(self):
        c = self.here
        return (1 - self.rep, c[X] * 16 + c[Y] * 4 + c[Z])

    def copy(self, src, dst, axis, by, send, recv):
        return pltpu.make_async_remote_copy(
            src_ref=src, dst_ref=dst, send_sem=send, recv_sem=recv, device_id=self.device(axis, by), device_id_type=MESH
        )

    def send(self, src, dst, axis, by, sems):
        copy = self.copy(src, dst, axis, by, sems[0].at[self.count], sems[1].at[self.count])
        self.count += 1
        copy.start()
        self.started.append(copy)
        return copy

    def parts(self):
        made = []
        for n in PARTS:
            p = Part()
            p.n, p.order = n, ORDERS[n]
            p.second = ORDERS[n][SECOND] < ORDERS[n][THIRD]
            made.append(p)
        return made

    def index(self, p, i, j, k):
        index = [None] * 3
        for a, value in zip(p.order, (i, j, k)):
            index[a] = slice(None) if value is None else value
        return tuple(index)


def step_kernel(*refs):
    grads, weights, m_in, v_in = (refs[i : i + 3] for i in (0, 3, 6, 9))
    new0, new1, mo, vo = refs[12:16]
    scratch = refs[16:]
    lines, scratch = scratch[:3], scratch[3:]
    own, scratch = [scratch[2 * n : 2 * n + 2] for n in PARTS], scratch[6:]
    packed, scratch = [scratch[2 * n : 2 * n + 2] for n in PARTS], scratch[6:]
    rec, scratch = [[scratch[18 * n + 6 * f : 18 * n + 6 * f + 6] for f in PARTS] for n in PARTS], scratch[54:]
    gs, sq, sqr, send, recv, early_send, early_recv, load_sem, go = scratch
    sems = (send, recv)

    place = Place((RIGHT, FAR, LEFT), True)
    ahead, behind = place.rep == 1, place.rep == 0
    at = place.at
    parts = place.parts()

    def line_copies(srcs, line, slot):
        for n, (src, height) in enumerate(zip(srcs, (40, 40, 200))):
            rows = pl.ds(pl.multiple_of(line * height, 8), height)
            yield pltpu.make_async_copy(src.at[:, rows, :], lines[n].at[slot], load_sem.at[slot, n])

    def pack(slot, outs):
        for n in PARTS:
            src = lines[n].at[slot]
            if n < 2:
                pack_wide(src, outs[n])
            else:
                pack_tall(src, outs[n])

    def distance(u):
        return lax.rem(6 - u + 3 * lax.div(u, 2) - 2 * lax.div(u, 3), 4)

    def where(t):
        u, w = lax.div(t, 4), lax.rem(t, 4)
        return w, lax.rem(u + w, 4)

    def line_of(t):
        a, b = where(t)
        return at(X, distance(a)), at(Y, distance(b))

    def start_line(t):
        x, y = line_of(t)
        for c in line_copies(grads, x * 4 + y, lax.rem(t, 2)):
            c.start()

    start_line(0)
    start_line(1)

    def early(p, s, src, dst, way):
        return place.copy(src, dst, p.order[FIRST], way, early_send.at[p.n, s], early_recv.at[p.n, s])

    def to_far(p, piece, block):
        for half, way in enumerate((RIGHT, LEFT)):
            early(p, half, packed[p.n][half].at[piece], rec[p.n][FIRST][half].at[block], way).start()

    def one_line(t):
        slot = lax.rem(t, 2)
        a, b = where(t)
        x, y = line_of(t)
        for c in line_copies(grads, x * 4 + y, slot):
            c.wait()
        pack(slot, [[half.at[x, y] for half in packed[n]] for n in PARTS])

        @pl.when(t < 14)
        def _():
            start_line(t + 2)

        @pl.when(a == 0)
        def _():
            to_far(parts[0], (x, y), y)

        @pl.when(b == 0)
        def _():
            to_far(parts[1], (x, y), x)

        to_far(parts[2], (x, y, at(Z, FAR)), (x, y))

    each(16, one_line)

    def whole_pieces(kinds):
        for p in parts:
            for s, half, by, way in kinds:
                piece = place.index(p, at(p.order[FIRST], by), None, None)
                early(p, s, packed[p.n][half].at[piece], rec[p.n][FIRST][s], way).start()

    NEAR_PIECES = ((2, 1, RIGHT, RIGHT), (3, 0, LEFT, LEFT))

    @pl.when(ahead)
    def _():
        whole_pieces(NEAR_PIECES)

    def early_sent():
        for p in parts:
            for s in RING:
                ref = rec[p.n][FIRST][s]
                early(p, s, ref, ref, LEFT).wait_send()

    for c in line_copies(weights, at(X, ME) * 4 + at(Y, ME), 0):
        c.start()
    for new, old in ((mo, m_in), (vo, v_in)):
        new[:, ROWS - TAIL : ROWS, :] = jnp.zeros((3, TAIL, LANES), F32)
        for n in PARTS:
            rows, height, tiles = (tall_rows, 50, 5) if n == 2 else (wide_rows, 10, 25)
            for tile in range(tiles):
                for s in LAYERS:
                    new[n, pl.ds(rows(tile, s), height), :] = old[n][:, s, tile * LANES : (tile + 1) * LANES]
    for c in line_copies(weights, at(X, ME) * 4 + at(Y, ME), 0):
        c.wait()
    pack(0, own)

    @pl.when(behind)
    def _():
        pl.semaphore_wait(go, 1)
        whole_pieces(NEAR_PIECES)

    def early_wait(p, s):
        ref = rec[p.n][FIRST][s]
        early(p, s, ref, ref, LEFT).wait_recv()

    def block(p, ref, j, k):
        return ref.at[(j, k) if p.second else (k, j)]

    def whole(p, ref, j):
        return ref.at[j] if p.second else ref.at[:, j]

    def total(refs):
        value = refs[0][...].astype(F32)
        for ref in refs[1:]:
            value = value + ref[...].astype(F32)
        return value

    def terms1(p, half, piece, j, k):
        return [packed[p.n][half].at[place.index(p, piece, j, k)]]

    def terms2(p, half, j, k):
        _, _, dir_l, dir_r, com_l, com_r = rec[p.n][FIRST]
        more = ((dir_r, com_l), (dir_l, com_r))[half]
        return terms1(p, half, p.me[FIRST], j, k) + [block(p, ref, j, k) for ref in more]

    def terms3(p, half, k):
        _, _, dir_l, dir_r, com_l, com_r = rec[p.n][SECOND]
        more = ((dir_r, com_l), (dir_l, com_r))[half]
        return terms2(p, half, p.me[SECOND], k) + [ref.at[k] for ref in more]

    STEPS = (FAR, RIGHT, LEFT, ME)
    LEAVES = {
        FAR: ((0, 3, 0, RIGHT), (1, 2, 1, LEFT)),
        RIGHT: ((1, 2, 2, RIGHT),),
        LEFT: ((0, 3, 3, LEFT),),
        ME: (),
    }
    COMBINE = ((0, 0, 4, RIGHT), (1, 1, 5, LEFT))

    for p in parts:
        p.me = [at(a, ME) for a in p.order]
        p.to = {by: [at(a, by) for a in p.order] for by in STEPS}
        early_wait(p, 0)
        early_wait(p, 1)
        p.com = {}
    for by in STEPS:
        for p in parts:
            j = p.to[by][SECOND]
            p.com[by] = []
            for half, got, to, way in COMBINE:
                got, to = (rec[p.n][FIRST][i] for i in (got, to))

                def add(k):
                    ref = block(p, got, j, k)
                    ref[...] = total(terms1(p, half, p.to[way][FIRST], j, k) + [ref]).astype(BF)

                each(SIDE, add)
                p.com[by].append(place.send(whole(p, got, j), whole(p, to, j), p.order[FIRST], way, sems))

    @pl.when(ahead)
    def _():
        early_sent()
        for c in place.started:
            c.wait_send()
        pl.semaphore_signal(go, inc=1, device_id=place.other_core(), device_id_type=MESH)

    for p in parts:
        early_wait(p, 2)
        early_wait(p, 3)
        p.next = {}

    for by in STEPS:
        for p in parts:
            j = p.to[by][SECOND]
            for c in p.com[by]:
                c.wait_recv()
            for half, slot, target, way in LEAVES[by]:
                ref = rec[p.n][FIRST][slot]

                def add(k):
                    block(p, ref, j, k)[...] = total(terms2(p, half, j, k)).astype(BF)

                each(SIDE, add)
                p.next[target] = place.send(whole(p, ref, j), rec[p.n][SECOND][target], p.order[SECOND], way, sems)

    for p in parts:
        p.next[0].wait_recv()
        p.next[1].wait_recv()
    for by in STEPS:
        for p in parts:
            k = p.to[by][THIRD]
            p.com[by] = []
            for half, got, to, way in COMBINE:
                got, to = (rec[p.n][SECOND][i].at[k] for i in (got, to))
                got[...] = total(terms2(p, half, p.to[way][SECOND], k) + [got]).astype(BF)
                p.com[by].append(place.send(got, to, p.order[SECOND], way, sems))
    for p in parts:
        p.next[2].wait_recv()
        p.next[3].wait_recv()
        p.next = {}

    for by in STEPS:
        for p in parts:
            k = p.to[by][THIRD]
            for c in p.com[by]:
                c.wait_recv()
            for half, slot, target, way in LEAVES[by]:
                ref = rec[p.n][SECOND][slot].at[k]
                ref[...] = total(terms3(p, half, k)).astype(BF)
                p.next[target] = place.send(ref, rec[p.n][THIRD][target], p.order[THIRD], way, sems)

    for p in parts:
        p.com = []
        for half, got, to, way in COMBINE:
            p.next[got].wait_recv()
            got, to = (rec[p.n][THIRD][i] for i in (got, to))
            got[...] = total(terms3(p, half, p.to[way][THIRD]) + [got]).astype(BF)
            p.com.append(place.send(got, to, p.order[THIRD], way, sems))
    squares = jnp.zeros((8, LANES), F32)
    for p in parts:
        for c in (p.next[2], p.next[3], *p.com):
            c.wait_recv()
        _, _, dir_l, dir_r, com_l, com_r = rec[p.n][THIRD]
        for half in LAYERS:
            g = total(terms3(p, half, p.me[THIRD]) + [(dir_r, dir_l)[half], (com_l, com_r)[half]]).astype(BF).astype(F32)
            gs[p.n, SPAN[half], :] = g
            squares += jnp.sum((g * g).reshape(-1, 8, LANES), axis=0)

    for axis in (X, Y, Z):
        sq[axis] = squares
        copies = [place.send(sq.at[axis], sqr.at[axis, i], axis, by, sems) for i, by in enumerate((RIGHT, FAR, LEFT))]
        for i, c in enumerate(copies):
            c.wait_recv()
            squares += sqr[axis, i]
    squares = jnp.sum(squares, axis=(0, 1), keepdims=True)
    factor = jnp.minimum(1.0, 0.5 * lax.rsqrt(squares / COUNT + 1e-30))

    for n in PARTS:
        for half in LAYERS:
            rows = SPAN[half]
            g = gs[n, rows, :] * factor
            w = own[n][half][at(Z, ME)].astype(F32)
            m = 0.9 * mo[n, rows, :] + 0.1 * g
            v = 0.95 * vo[n, rows, :] + 0.05 * g * g
            mo[n, rows, :] = m
            vo[n, rows, :] = v
            (new0, new1)[half][n] = (w - 0.02 * (m * lax.rsqrt(v + 1e-8) + 0.1 * w)).astype(BF)

    for c in place.started[24:]:
        c.wait_send()

    @pl.when(behind)
    def _():
        early_sent()
        for c in place.started[:24]:
            c.wait_send()


def halves(*lead, dtype=BF):
    return [pltpu.VMEM((*lead, h, LANES), dtype) for h in HALF]


def shape(*dims, dtype=BF):
    return jax.ShapeDtypeStruct(dims, dtype)


def step(grads, weights, m, v):
    rec = []
    for lead in ((4, 4), (4,), ()):
        a, b = halves(*lead)
        rec += [a, b, b, a, a, b]
    copies = 87
    return pl.pallas_call(
        step_kernel,
        out_shape=[shape(3, HALF[0], LANES), shape(3, HALF[1], LANES)] + [shape(3, ROWS, LANES, dtype=F32)] * 2,
        in_specs=[ANY] * 6 + [VM] * 6,
        out_specs=[VM] * 4,
        scratch_shapes=[
            pltpu.VMEM((2, 2, 40, 3200), BF),
            pltpu.VMEM((2, 2, 40, 3200), BF),
            pltpu.VMEM((2, 2, 200, 640), BF),
            *halves(4) * 3,
            *halves(*GRID) * 3,
            *rec * 3,
            pltpu.VMEM((3, ROWS, LANES), F32),
            pltpu.VMEM((3, 8, LANES), F32),
            pltpu.VMEM((3, 3, 8, LANES), F32),
            pltpu.SemaphoreType.DMA((copies,)),
            pltpu.SemaphoreType.DMA((copies,)),
            pltpu.SemaphoreType.DMA((3, 4)),
            pltpu.SemaphoreType.DMA((3, 4)),
            pltpu.SemaphoreType.DMA((2, 3)),
            pltpu.SemaphoreType.REGULAR,
        ],
        compiler_params=pltpu.CompilerParams(collective_id=0, has_side_effects=True, vmem_limit_bytes=67043328),
        name="step",
    )(*grads, *weights, *m, *v)


def gather_kernel(*refs):
    new, moments, outs, moved = (refs[i:j] for i, j in ((0, 2), (2, 4), (4, 7), (7, 13)))
    scratch = refs[13:]
    got = [scratch[2 * n : 2 * n + 2] for n in PARTS]
    send, recv, late_send, late_recv = scratch[6:]
    sems = (send, recv)

    place = Place((RIGHT, LEFT))
    at = place.at
    parts = place.parts()
    for p in parts:
        p.me, p.left, p.right, p.far = ([at(a, by) for a in p.order] for by in (ME, LEFT, RIGHT, FAR))
        p.steps = (p.me, p.left, p.right, p.far)

    def ref_of(p, half, i, j, k):
        return got[p.n][half].at[place.index(p, i, j, k)]

    def spread(p, axis, i, j, k, mine=False):
        to = [ref_of(p, h, i, j, k) for h in LAYERS]
        src = [new[h].at[p.n] for h in LAYERS] if mine else to
        return [place.send(src[h], to[h], axis, by, sems) for h, by in ((0, RIGHT), (1, LEFT), (1, RIGHT), (0, LEFT))]

    def forward(p, axis, copies, from_left, from_right):
        copies[0].wait_recv()
        left = ref_of(p, 0, *from_left)
        a = place.send(left, left, axis, RIGHT, sems)
        copies[1].wait_recv()
        right = ref_of(p, 1, *from_right)
        return a, place.send(right, right, axis, LEFT, sems)

    def arrived(*copies):
        for c in copies:
            c.wait_recv()

    def chunk(p, axis_place, step):
        i, value = axis_place, step
        return (i, None, value) if p.n == 1 else (i, value, None)

    def late(p, jj, e, half, index, way):
        ref = ref_of(p, half, *index)
        return place.copy(ref, ref, p.order[FIRST], way, late_send.at[p.n, jj, e], late_recv.at[p.n, jj, e])

    def along(p):
        return p.order[THIRD if p.n == 1 else SECOND]

    def last_spread(p, j, k):
        jj = ORDER.index(k if p.n == 1 else j)
        mine = j == ME and k == ME
        index = (p.me[FIRST], at(p.order[SECOND], j), at(p.order[THIRD], k))
        for e, (h, way) in enumerate(((0, RIGHT), (1, LEFT), (1, RIGHT), (0, LEFT))):
            to = ref_of(p, h, *index)
            sems = late_send.at[p.n, jj, e], late_recv.at[p.n, jj, e]
            place.copy(new[h].at[p.n] if mine else to, to, p.order[FIRST], way, *sems).start()

    for p in parts:
        p.s3 = spread(p, p.order[THIRD], *p.me, mine=True)
    for p in parts:
        p.s2, p.f2 = [spread(p, p.order[SECOND], *p.me, mine=True)], []
    for p in parts:
        last_spread(p, ME, ME)
    for p in parts:
        for h in LAYERS:
            ref_of(p, h, *p.me)[...] = new[h][p.n]
    for p in parts:
        i, j, k = p.me
        p.f3 = forward(p, p.order[THIRD], p.s3, (i, j, p.left[THIRD]), (i, j, p.right[THIRD]))
    for p in parts:
        arrived(*p.s3[2:])
        for k in (p.left[THIRD], p.right[THIRD]):
            p.s2.append(spread(p, p.order[SECOND], *p.me[:THIRD], k))
    for p in parts:
        last_spread(p, ME, LEFT)
        last_spread(p, ME, RIGHT)
    for p in parts:
        arrived(*p.f3)
        p.s2.append(spread(p, p.order[SECOND], *p.me[:THIRD], p.far[THIRD]))
        last_spread(p, ME, FAR)
    for step, by in enumerate((*ORDER, None)):
        for p in parts:
            if by is not None:
                i, k = p.me[FIRST], p.steps[step][THIRD]
                p.f2.append(forward(p, p.order[SECOND], p.s2[step], (i, p.left[SECOND], k), (i, p.right[SECOND], k)))
        for p in parts:
            if by is not None:
                arrived(*p.s2[step][2:])
                last_spread(p, LEFT, by)
                last_spread(p, RIGHT, by)
            if step:
                arrived(*p.f2[step - 1])
                last_spread(p, FAR, ORDER[step - 1])

    for out, one in zip((moved[:3], moved[3:]), moments):
        for n in PARTS:
            rows, height, tiles = (tall_rows, 50, 5) if n == 2 else (wide_rows, 10, 25)
            for tile in range(tiles):
                for s in LAYERS:
                    out[n][:, s, tile * LANES : (tile + 1) * LANES] = one[n, pl.ds(rows(tile, s), height), :]


    def line(p, x, y):
        block = [half.at[x, y] for half in got[p.n]]
        height = 200 if p.n == 2 else 40
        rows = pl.ds(pl.multiple_of((x * 4 + y) * height, 8), height)

        def write(layer, columns, value):
            outs[p.n][layer, rows, columns] = value.astype(BF)

        if p.n == 2:
            unpack_tall(block, write)
        else:
            unpack_wide(block, write)

    def distance(jj):
        return 3 * lax.rem(jj, 2) + lax.div(jj, 2) - 2 * lax.div(jj, 3)

    def last(jj):
        @pl.when(jj < 4)
        def _():
            for p in parts:
                value = at(along(p), distance(jj))
                left, right = (chunk(p, i, value) for i in (p.left[FIRST], p.right[FIRST]))
                late(p, jj, 0, 0, left, LEFT).wait_recv()
                late(p, jj, 4, 0, left, RIGHT).start()
                late(p, jj, 1, 1, right, LEFT).wait_recv()
                late(p, jj, 5, 1, right, LEFT).start()
            for p in parts:
                value = at(along(p), distance(jj))
                left, right = (chunk(p, i, value) for i in (p.left[FIRST], p.right[FIRST]))
                late(p, jj, 2, 1, left, LEFT).wait_recv()
                late(p, jj, 3, 0, right, LEFT).wait_recv()

        before = jj - LAG

        @pl.when(jj >= LAG)
        def _():
            for p in parts:
                far = chunk(p, p.far[FIRST], at(along(p), distance(before)))
                late(p, before, 4, 0, far, LEFT).wait_recv()
                late(p, before, 5, 1, far, LEFT).wait_recv()

        def one(i):
            which = jj - LAG * lax.div(i, 3)

            @pl.when((which >= 0) & (which < 4))
            def _():
                value = distance(which)
                line(parts[0], at(X, distance(i)), at(Y, value))
                line(parts[1], at(X, value), at(Y, distance(i)))

            @pl.when(jj >= LAG)
            def _():
                line(parts[2], at(X, distance(before)), i)

        each(SIDE, one)

    each(SIDE + LAG, last)

    for c in place.started:
        c.wait_send()

    def drain(jj):
        for p in parts:
            index = chunk(p, p.me[FIRST], at(along(p), distance(jj)))
            for e, h in enumerate((0, 1, 1, 0, 0, 1)):
                late(p, jj, e, h, index, LEFT).wait_send()

    each(SIDE, drain)


def gather(new, moments):
    copies = 90
    wide, tall = (10, 2, 3200), (50, 2, 640)
    outs = [pltpu.VMEM((2, 640, 3200), BF)] * 2 + [pltpu.VMEM((2, 3200, 640), BF)]
    outs += [pltpu.VMEM(one, F32) for one in (wide, wide, tall)] * 2
    return pl.pallas_call(
        gather_kernel,
        out_shape=outs,
        in_specs=[VM] * 4,
        out_specs=[VM] * MANY,
        scratch_shapes=[
            *halves(*GRID) * 3,
            pltpu.SemaphoreType.DMA((copies,)),
            pltpu.SemaphoreType.DMA((copies,)),
            pltpu.SemaphoreType.DMA((3, 4, 6)),
            pltpu.SemaphoreType.DMA((3, 4, 6)),
        ],
        compiler_params=pltpu.CompilerParams(collective_id=1, has_side_effects=True, vmem_limit_bytes=30 * 2**20),
        name="gather",
    )(*new, *moments)


def finish_kernel(*refs):
    held, outs, sem = refs[:MANY], refs[MANY : 2 * MANY], refs[2 * MANY]
    copies = [pltpu.make_async_copy(a, b, sem.at[n]) for n, (a, b) in enumerate(zip(held, outs))]
    for c in copies:
        c.start()
    for c in copies:
        c.wait()


def finish(held):
    return pl.pallas_call(
        finish_kernel,
        out_shape=[shape(*one.shape, dtype=one.dtype) for one in held],
        in_specs=[VM] * MANY,
        out_specs=[ANY] * MANY,
        scratch_shapes=[pltpu.SemaphoreType.DMA((MANY,))],
        compiler_params=pltpu.CompilerParams(vmem_limit_bytes=8 * 2**20),
        name="finish",
    )(*held)


def solution(mesh):
    def run(*arrays):
        terms, weights, m, v = (arrays[i : i + 3] for i in (0, 3, 6, 9))
        swap = lambda arrays: [x.transpose(1, 0, 2) for x in arrays]
        *new, mo, vo = step([t[0] for t in terms], weights, swap(m), swap(v))
        outs = finish(gather(new, (mo, vo)))
        return (*outs[:3], *swap(outs[3:]))

    all_of, cut = P(None, None, None), P(None, "dp", None)
    return jax.shard_map(
        run,
        mesh=mesh,
        in_specs=(P(("rep", "dp"), None, None, None),) * 3 + (all_of,) * 3 + (cut,) * 6,
        out_specs=(P("rep", None, None),) * 3 + (P("rep", "dp", None),) * 6,
        check_vma=False,
    )
```

```python
import jax
import jax.numpy as jnp
from jax import lax
from jax.experimental import pallas as pl
from jax.experimental.pallas import tpu as pltpu
from jax.sharding import PartitionSpec as P

MESH = pl.DeviceIdType.MESH
BF, F32 = jnp.bfloat16, jnp.float32
ANY = pl.BlockSpec(memory_space=pl.ANY)
VM = pl.BlockSpec(memory_space=pltpu.VMEM)
LANES = 128
X, Y, Z = range(3)
FIRST, SECOND, THIRD = range(3)
LEFT, RIGHT, FAR, ME = -1, 1, 2, 0
LAYERS = (0, 1)
COUNT = 3 * 2 * 640 * 3200

ROWS = 504
HALF = (256, 248)
SPAN = (pl.ds(0, 256), pl.ds(256, 248))
QUAD, TAIL = 80, 24
GROUPS = [range(t, min(t + 4, 25)) for t in range(0, 25, 4)]
ORDERS = ((X, Y, Z), (Y, Z, X), (Z, X, Y))
PARTS = range(3)
MANY = 9
LAG = 2
ORDER = (ME, LEFT, RIGHT, FAR)
SIDE, RING, GRID = 4, range(4), (4, 4, 4)


def wide_rows(tile, layer):
    return tile * 20 + layer * 10


def tall_rows(tile, layer):
    return tile * 100 + layer * 50


def stack(values, axis=0):
    return jnp.concatenate(values, axis=axis)


def put(out, z, first, value):
    cut = HALF[0]
    end = first + value.shape[0]
    value = value.astype(BF) if first >= cut or end <= cut else value
    if first >= cut:
        out[1][z, first - cut : end - cut, :] = value
    elif end <= cut:
        out[0][z, first:end, :] = value
    else:
        out[0][z, first:cut, :] = value[: cut - first].astype(BF)
        out[1][z, : end - cut, :] = value[cut - first :].astype(BF)


def get(ref, z, first, end):
    cut = HALF[0]
    low, high = first // 16 * 16, -(-end // 16) * 16
    if low >= cut:
        value = ref[1][z, low - cut : min(high, ROWS) - cut, :].astype(F32)
    elif high <= cut:
        value = ref[0][z, low:high, :].astype(F32)
    else:
        value = stack([ref[0][z, low:cut, :].astype(F32), ref[1][z, : min(high, ROWS) - cut, :].astype(F32)])
    return value[first - low : end - low]


def pack_wide(src, out):
    for group in range(7):
        tiles = GROUPS[group]
        x = [[src[s, :, pl.ds(t * LANES, LANES)].astype(F32) for s in LAYERS] for t in tiles]
        for z in RING:
            rows = [one[s][z * 10 : (z + 1) * 10] for one in x for s in LAYERS]
            if len(tiles) == 1:
                rows.append(jnp.zeros((SIDE, LANES), F32))
            put(out, z, group * QUAD, stack(rows))


def unpack_wide(block, write):
    for group in range(7):
        tiles = GROUPS[group]
        got = [get(block, z, group * QUAD, min(ROWS, (group + 1) * QUAD)) for z in RING]
        for n, t in enumerate(tiles):
            for s in LAYERS:
                row = n * 20 + s * 10
                write(s, pl.ds(t * LANES, LANES), stack([one[row : row + 10] for one in got]))


def pack_tall(src, out):
    x = [[src[s, :, pl.ds(t * LANES, LANES)].astype(F32) for s in LAYERS] for t in range(5)]
    for z in RING:
        rows = [one[s][z * 50 : (z + 1) * 50] for one in x for s in LAYERS]
        put(out, z, 0, stack([*rows, jnp.zeros((SIDE, LANES), F32)]))


def unpack_tall(block, write):
    got = [get(block, z, 0, ROWS) for z in RING]
    for t in range(5):
        for s in LAYERS:
            row = tall_rows(t, s)
            write(s, pl.ds(t * LANES, LANES), stack([one[row : row + 50] for one in got]))


def each(count, body, start=0):
    lax.fori_loop(start, count, lambda i, _: (body(i), None)[1], None)


class Part:
    pass


class Place:
    def __init__(self, partners, other_core=False):
        self.rep, dp = lax.axis_index("rep"), lax.axis_index("dp")
        self.here = (lax.div(dp, 16), lax.rem(lax.div(dp, 4), 4), lax.rem(dp, 4))
        barrier = pltpu.get_barrier_semaphore()
        for axis in (X, Y, Z):
            for by in partners:
                pl.semaphore_signal(barrier, inc=1, device_id=self.device(axis, by), device_id_type=MESH)
        if other_core:
            pl.semaphore_signal(barrier, inc=1, device_id=self.other_core(), device_id_type=MESH)
        self.barrier, self.greeted = barrier, 3 * len(partners) + other_core
        self.count = 0
        self.started = []

    def at(self, axis, by):
        return lax.rem(self.here[axis] + (by + 4), 4)

    def device(self, axis, by):
        c = [self.at(a, by if a == axis else ME) for a in (X, Y, Z)]
        return (self.rep, c[X] * 16 + c[Y] * 4 + c[Z])

    def wait(self):
        pl.semaphore_wait(self.barrier, self.greeted)

    def other_core(self):
        c = self.here
        return (1 - self.rep, c[X] * 16 + c[Y] * 4 + c[Z])

    def copy(self, src, dst, axis, by, send, recv):
        return pltpu.make_async_remote_copy(
            src_ref=src, dst_ref=dst, send_sem=send, recv_sem=recv, device_id=self.device(axis, by), device_id_type=MESH
        )

    def send(self, src, dst, axis, by, sems):
        copy = self.copy(src, dst, axis, by, sems[0].at[self.count], sems[1].at[self.count])
        self.count += 1
        copy.start()
        self.started.append(copy)
        return copy

    def parts(self):
        made = []
        for n in PARTS:
            p = Part()
            p.n, p.order = n, ORDERS[n]
            p.second = ORDERS[n][SECOND] < ORDERS[n][THIRD]
            made.append(p)
        return made

    def index(self, p, i, j, k):
        index = [None] * 3
        for a, value in zip(p.order, (i, j, k)):
            index[a] = slice(None) if value is None else value
        return tuple(index)


def step_kernel(*refs):
    grads, weights, m_in, v_in = (refs[i : i + 3] for i in (0, 3, 6, 9))
    new0, new1, mo, vo = refs[12:16]
    scratch = refs[16:]
    lines, scratch = scratch[:3], scratch[3:]
    own, scratch = [scratch[2 * n : 2 * n + 2] for n in PARTS], scratch[6:]
    packed, scratch = [scratch[2 * n : 2 * n + 2] for n in PARTS], scratch[6:]
    rec, scratch = [[scratch[18 * n + 6 * f : 18 * n + 6 * f + 6] for f in PARTS] for n in PARTS], scratch[54:]
    gs, sq, sqr, send, recv, early_send, early_recv, load_sem, go = scratch
    sems = (send, recv)

    place = Place((RIGHT, FAR, LEFT), True)
    ahead, behind = place.rep == 1, place.rep == 0
    at = place.at
    parts = place.parts()

    def line_copies(srcs, line, slot):
        for n, (src, height) in enumerate(zip(srcs, (40, 40, 200))):
            rows = pl.ds(pl.multiple_of(line * height, 8), height)
            yield pltpu.make_async_copy(src.at[:, rows, :], lines[n].at[slot], load_sem.at[slot, n])

    def pack(slot, outs):
        for n in PARTS:
            src = lines[n].at[slot]
            if n < 2:
                pack_wide(src, outs[n])
            else:
                pack_tall(src, outs[n])

    def distance(u):
        return lax.rem(6 - u + 3 * lax.div(u, 2) - 2 * lax.div(u, 3), 4)

    def where(t):
        u, w = lax.div(t, 4), lax.rem(t, 4)
        return w, lax.rem(u + w, 4)

    def line_of(t):
        a, b = where(t)
        return at(X, distance(a)), at(Y, distance(b))

    def start_line(t):
        x, y = line_of(t)
        for c in line_copies(grads, x * 4 + y, lax.rem(t, 2)):
            c.start()

    start_line(0)
    start_line(1)

    def early(p, s, src, dst, way):
        return place.copy(src, dst, p.order[FIRST], way, early_send.at[p.n, s], early_recv.at[p.n, s])

    def to_far(p, piece, block):
        for half, way in enumerate((RIGHT, LEFT)):
            early(p, half, packed[p.n][half].at[piece], rec[p.n][FIRST][half].at[block], way).start()

    def one_line(t, first=False):
        slot = lax.rem(t, 2)
        a, b = where(t)
        x, y = line_of(t)
        for c in line_copies(grads, x * 4 + y, slot):
            c.wait()
        pack(slot, [[half.at[x, y] for half in packed[n]] for n in PARTS])

        @pl.when(t < 14)
        def _():
            start_line(t + 2)

        if first:
            place.wait()

        @pl.when(a == 0)
        def _():
            to_far(parts[0], (x, y), y)

        @pl.when(b == 0)
        def _():
            to_far(parts[1], (x, y), x)

        to_far(parts[2], (x, y, at(Z, FAR)), (x, y))

    one_line(0, True)
    each(16, one_line, start=1)

    def whole_pieces(kinds):
        for p in parts:
            for s, half, by, way in kinds:
                piece = place.index(p, at(p.order[FIRST], by), None, None)
                early(p, s, packed[p.n][half].at[piece], rec[p.n][FIRST][s], way).start()

    NEAR_PIECES = ((2, 1, RIGHT, RIGHT), (3, 0, LEFT, LEFT))

    @pl.when(ahead)
    def _():
        whole_pieces(NEAR_PIECES)

    def early_sent():
        for p in parts:
            for s in RING:
                ref = rec[p.n][FIRST][s]
                early(p, s, ref, ref, LEFT).wait_send()

    for c in line_copies(weights, at(X, ME) * 4 + at(Y, ME), 0):
        c.start()
    for new, old in ((mo, m_in), (vo, v_in)):
        new[:, ROWS - TAIL : ROWS, :] = jnp.zeros((3, TAIL, LANES), F32)
        for n in PARTS:
            rows, height, tiles = (tall_rows, 50, 5) if n == 2 else (wide_rows, 10, 25)
            for tile in range(tiles):
                for s in LAYERS:
                    new[n, pl.ds(rows(tile, s), height), :] = old[n][:, s, tile * LANES : (tile + 1) * LANES]
    for c in line_copies(weights, at(X, ME) * 4 + at(Y, ME), 0):
        c.wait()
    pack(0, own)

    @pl.when(behind)
    def _():
        pl.semaphore_wait(go, 1)
        whole_pieces(NEAR_PIECES)

    def early_wait(p, s):
        ref = rec[p.n][FIRST][s]
        early(p, s, ref, ref, LEFT).wait_recv()

    def block(p, ref, j, k):
        return ref.at[(j, k) if p.second else (k, j)]

    def whole(p, ref, j):
        return ref.at[j] if p.second else ref.at[:, j]

    def total(refs):
        value = refs[0][...].astype(F32)
        for ref in refs[1:]:
            value = value + ref[...].astype(F32)
        return value

    def terms1(p, half, piece, j, k):
        return [packed[p.n][half].at[place.index(p, piece, j, k)]]

    def terms2(p, half, j, k):
        _, _, dir_l, dir_r, com_l, com_r = rec[p.n][FIRST]
        more = ((dir_r, com_l), (dir_l, com_r))[half]
        return terms1(p, half, p.me[FIRST], j, k) + [block(p, ref, j, k) for ref in more]

    def terms3(p, half, k):
        _, _, dir_l, dir_r, com_l, com_r = rec[p.n][SECOND]
        more = ((dir_r, com_l), (dir_l, com_r))[half]
        return terms2(p, half, p.me[SECOND], k) + [ref.at[k] for ref in more]

    STEPS = (FAR, RIGHT, LEFT, ME)
    LEAVES = {
        FAR: ((0, 3, 0, RIGHT), (1, 2, 1, LEFT)),
        RIGHT: ((1, 2, 2, RIGHT),),
        LEFT: ((0, 3, 3, LEFT),),
        ME: (),
    }
    COMBINE = ((0, 0, 4, RIGHT), (1, 1, 5, LEFT))

    for p in parts:
        p.me = [at(a, ME) for a in p.order]
        p.to = {by: [at(a, by) for a in p.order] for by in STEPS}
        early_wait(p, 0)
        early_wait(p, 1)
        p.com = {}
    for by in STEPS:
        for p in parts:
            j = p.to[by][SECOND]
            p.com[by] = []
            for half, got, to, way in COMBINE:
                got, to = (rec[p.n][FIRST][i] for i in (got, to))

                def add(k):
                    ref = block(p, got, j, k)
                    ref[...] = total(terms1(p, half, p.to[way][FIRST], j, k) + [ref]).astype(BF)

                each(SIDE, add)
                p.com[by].append(place.send(whole(p, got, j), whole(p, to, j), p.order[FIRST], way, sems))

    @pl.when(ahead)
    def _():
        early_sent()
        for c in place.started:
            c.wait_send()
        pl.semaphore_signal(go, inc=1, device_id=place.other_core(), device_id_type=MESH)

    for p in parts:
        early_wait(p, 2)
        early_wait(p, 3)
        p.next = {}

    for by in STEPS:
        for p in parts:
            j = p.to[by][SECOND]
            for c in p.com[by]:
                c.wait_recv()
            for half, slot, target, way in LEAVES[by]:
                ref = rec[p.n][FIRST][slot]

                def add(k):
                    block(p, ref, j, k)[...] = total(terms2(p, half, j, k)).astype(BF)

                each(SIDE, add)
                p.next[target] = place.send(whole(p, ref, j), rec[p.n][SECOND][target], p.order[SECOND], way, sems)

    for p in parts:
        p.next[0].wait_recv()
        p.next[1].wait_recv()
    for by in STEPS:
        for p in parts:
            k = p.to[by][THIRD]
            p.com[by] = []
            for half, got, to, way in COMBINE:
                got, to = (rec[p.n][SECOND][i].at[k] for i in (got, to))
                got[...] = total(terms2(p, half, p.to[way][SECOND], k) + [got]).astype(BF)
                p.com[by].append(place.send(got, to, p.order[SECOND], way, sems))
    for p in parts:
        p.next[2].wait_recv()
        p.next[3].wait_recv()
        p.next = {}

    for by in STEPS:
        for p in parts:
            k = p.to[by][THIRD]
            for c in p.com[by]:
                c.wait_recv()
            for half, slot, target, way in LEAVES[by]:
                ref = rec[p.n][SECOND][slot].at[k]
                ref[...] = total(terms3(p, half, k)).astype(BF)
                p.next[target] = place.send(ref, rec[p.n][THIRD][target], p.order[THIRD], way, sems)

    for p in parts:
        p.com = []
        for half, got, to, way in COMBINE:
            p.next[got].wait_recv()
            got, to = (rec[p.n][THIRD][i] for i in (got, to))
            got[...] = total(terms3(p, half, p.to[way][THIRD]) + [got]).astype(BF)
            p.com.append(place.send(got, to, p.order[THIRD], way, sems))
    squares = jnp.zeros((8, LANES), F32)
    for p in parts:
        for c in (p.next[2], p.next[3], *p.com):
            c.wait_recv()
        _, _, dir_l, dir_r, com_l, com_r = rec[p.n][THIRD]
        for half in LAYERS:
            g = total(terms3(p, half, p.me[THIRD]) + [(dir_r, dir_l)[half], (com_l, com_r)[half]]).astype(BF).astype(F32)
            gs[p.n, SPAN[half], :] = g
            squares += jnp.sum((g * g).reshape(-1, 8, LANES), axis=0)

    for axis in (X, Y, Z):
        sq[axis] = squares
        copies = [place.send(sq.at[axis], sqr.at[axis, i], axis, by, sems) for i, by in enumerate((RIGHT, FAR, LEFT))]
        for i, c in enumerate(copies):
            c.wait_recv()
            squares += sqr[axis, i]
    squares = jnp.sum(squares, axis=(0, 1), keepdims=True)
    factor = jnp.minimum(1.0, 0.5 * lax.rsqrt(squares / COUNT + 1e-30))

    for n in PARTS:
        for half in LAYERS:
            rows = SPAN[half]
            g = gs[n, rows, :] * factor
            w = own[n][half][at(Z, ME)].astype(F32)
            m = 0.9 * mo[n, rows, :] + 0.1 * g
            v = 0.95 * vo[n, rows, :] + 0.05 * g * g
            mo[n, rows, :] = m
            vo[n, rows, :] = v
            (new0, new1)[half][n] = (w - 0.02 * (m * lax.rsqrt(v + 1e-8) + 0.1 * w)).astype(BF)

    for c in place.started[24:]:
        c.wait_send()

    @pl.when(behind)
    def _():
        early_sent()
        for c in place.started[:24]:
            c.wait_send()


def halves(*lead, dtype=BF):
    return [pltpu.VMEM((*lead, h, LANES), dtype) for h in HALF]


def shape(*dims, dtype=BF):
    return jax.ShapeDtypeStruct(dims, dtype)


def step(grads, weights, m, v):
    rec = []
    for lead in ((4, 4), (4,), ()):
        a, b = halves(*lead)
        rec += [a, b, b, a, a, b]
    copies = 87
    return pl.pallas_call(
        step_kernel,
        out_shape=[shape(3, HALF[0], LANES), shape(3, HALF[1], LANES)] + [shape(3, ROWS, LANES, dtype=F32)] * 2,
        in_specs=[ANY] * 6 + [VM] * 6,
        out_specs=[VM] * 4,
        scratch_shapes=[
            pltpu.VMEM((2, 2, 40, 3200), BF),
            pltpu.VMEM((2, 2, 40, 3200), BF),
            pltpu.VMEM((2, 2, 200, 640), BF),
            *halves(4) * 3,
            *halves(*GRID) * 3,
            *rec * 3,
            pltpu.VMEM((3, ROWS, LANES), F32),
            pltpu.VMEM((3, 8, LANES), F32),
            pltpu.VMEM((3, 3, 8, LANES), F32),
            pltpu.SemaphoreType.DMA((copies,)),
            pltpu.SemaphoreType.DMA((copies,)),
            pltpu.SemaphoreType.DMA((3, 4)),
            pltpu.SemaphoreType.DMA((3, 4)),
            pltpu.SemaphoreType.DMA((2, 3)),
            pltpu.SemaphoreType.REGULAR,
        ],
        compiler_params=pltpu.CompilerParams(collective_id=0, has_side_effects=True, vmem_limit_bytes=67043328),
        name="step",
    )(*grads, *weights, *m, *v)


def gather_kernel(*refs):
    new, moments, outs, moved = (refs[i:j] for i, j in ((0, 2), (2, 4), (4, 7), (7, 13)))
    scratch = refs[13:]
    got = [scratch[2 * n : 2 * n + 2] for n in PARTS]
    send, recv, late_send, late_recv = scratch[6:]
    sems = (send, recv)

    place = Place((RIGHT, LEFT))
    place.wait()
    at = place.at
    parts = place.parts()
    for p in parts:
        p.me, p.left, p.right, p.far = ([at(a, by) for a in p.order] for by in (ME, LEFT, RIGHT, FAR))
        p.steps = (p.me, p.left, p.right, p.far)

    def ref_of(p, half, i, j, k):
        return got[p.n][half].at[place.index(p, i, j, k)]

    def spread(p, axis, i, j, k, mine=False):
        to = [ref_of(p, h, i, j, k) for h in LAYERS]
        src = [new[h].at[p.n] for h in LAYERS] if mine else to
        return [place.send(src[h], to[h], axis, by, sems) for h, by in ((0, RIGHT), (1, LEFT), (1, RIGHT), (0, LEFT))]

    def forward(p, axis, copies, from_left, from_right):
        copies[0].wait_recv()
        left = ref_of(p, 0, *from_left)
        a = place.send(left, left, axis, RIGHT, sems)
        copies[1].wait_recv()
        right = ref_of(p, 1, *from_right)
        return a, place.send(right, right, axis, LEFT, sems)

    def arrived(*copies):
        for c in copies:
            c.wait_recv()

    def chunk(p, axis_place, step):
        i, value = axis_place, step
        return (i, None, value) if p.n == 1 else (i, value, None)

    def late(p, jj, e, half, index, way):
        ref = ref_of(p, half, *index)
        return place.copy(ref, ref, p.order[FIRST], way, late_send.at[p.n, jj, e], late_recv.at[p.n, jj, e])

    def along(p):
        return p.order[THIRD if p.n == 1 else SECOND]

    def last_spread(p, j, k):
        jj = ORDER.index(k if p.n == 1 else j)
        mine = j == ME and k == ME
        index = (p.me[FIRST], at(p.order[SECOND], j), at(p.order[THIRD], k))
        for e, (h, way) in enumerate(((0, RIGHT), (1, LEFT), (1, RIGHT), (0, LEFT))):
            to = ref_of(p, h, *index)
            sems = late_send.at[p.n, jj, e], late_recv.at[p.n, jj, e]
            place.copy(new[h].at[p.n] if mine else to, to, p.order[FIRST], way, *sems).start()

    for p in parts:
        p.s3 = spread(p, p.order[THIRD], *p.me, mine=True)
    for p in parts:
        p.s2, p.f2 = [spread(p, p.order[SECOND], *p.me, mine=True)], []
    for p in parts:
        last_spread(p, ME, ME)
    for p in parts:
        for h in LAYERS:
            ref_of(p, h, *p.me)[...] = new[h][p.n]
    for p in parts:
        i, j, k = p.me
        p.f3 = forward(p, p.order[THIRD], p.s3, (i, j, p.left[THIRD]), (i, j, p.right[THIRD]))
    for p in parts:
        arrived(*p.s3[2:])
        for k in (p.left[THIRD], p.right[THIRD]):
            p.s2.append(spread(p, p.order[SECOND], *p.me[:THIRD], k))
    for p in parts:
        last_spread(p, ME, LEFT)
        last_spread(p, ME, RIGHT)
    for p in parts:
        arrived(*p.f3)
        p.s2.append(spread(p, p.order[SECOND], *p.me[:THIRD], p.far[THIRD]))
        last_spread(p, ME, FAR)
    for step, by in enumerate((*ORDER, None)):
        for p in parts:
            if by is not None:
                i, k = p.me[FIRST], p.steps[step][THIRD]
                p.f2.append(forward(p, p.order[SECOND], p.s2[step], (i, p.left[SECOND], k), (i, p.right[SECOND], k)))
        for p in parts:
            if by is not None:
                arrived(*p.s2[step][2:])
                last_spread(p, LEFT, by)
                last_spread(p, RIGHT, by)
            if step:
                arrived(*p.f2[step - 1])
                last_spread(p, FAR, ORDER[step - 1])

    for out, one in zip((moved[:3], moved[3:]), moments):
        for n in PARTS:
            rows, height, tiles = (tall_rows, 50, 5) if n == 2 else (wide_rows, 10, 25)
            for tile in range(tiles):
                for s in LAYERS:
                    out[n][:, s, tile * LANES : (tile + 1) * LANES] = one[n, pl.ds(rows(tile, s), height), :]


    def line(p, x, y):
        block = [half.at[x, y] for half in got[p.n]]
        height = 200 if p.n == 2 else 40
        rows = pl.ds(pl.multiple_of((x * 4 + y) * height, 8), height)

        def write(layer, columns, value):
            outs[p.n][layer, rows, columns] = value.astype(BF)

        if p.n == 2:
            unpack_tall(block, write)
        else:
            unpack_wide(block, write)

    def distance(jj):
        return 3 * lax.rem(jj, 2) + lax.div(jj, 2) - 2 * lax.div(jj, 3)

    def last(jj):
        @pl.when(jj < 4)
        def _():
            for p in parts:
                value = at(along(p), distance(jj))
                left, right = (chunk(p, i, value) for i in (p.left[FIRST], p.right[FIRST]))
                late(p, jj, 0, 0, left, LEFT).wait_recv()
                late(p, jj, 4, 0, left, RIGHT).start()
                late(p, jj, 1, 1, right, LEFT).wait_recv()
                late(p, jj, 5, 1, right, LEFT).start()
            for p in parts:
                value = at(along(p), distance(jj))
                left, right = (chunk(p, i, value) for i in (p.left[FIRST], p.right[FIRST]))
                late(p, jj, 2, 1, left, LEFT).wait_recv()
                late(p, jj, 3, 0, right, LEFT).wait_recv()

        before = jj - LAG

        @pl.when(jj >= LAG)
        def _():
            for p in parts:
                far = chunk(p, p.far[FIRST], at(along(p), distance(before)))
                late(p, before, 4, 0, far, LEFT).wait_recv()
                late(p, before, 5, 1, far, LEFT).wait_recv()

        def one(i):
            which = jj - LAG * lax.div(i, 3)

            @pl.when((which >= 0) & (which < 4))
            def _():
                value = distance(which)
                line(parts[0], at(X, distance(i)), at(Y, value))
                line(parts[1], at(X, value), at(Y, distance(i)))

            @pl.when(jj >= LAG)
            def _():
                line(parts[2], at(X, distance(before)), i)

        each(SIDE, one)

    each(SIDE + LAG, last)

    for c in place.started:
        c.wait_send()

    def drain(jj):
        for p in parts:
            index = chunk(p, p.me[FIRST], at(along(p), distance(jj)))
            for e, h in enumerate((0, 1, 1, 0, 0, 1)):
                late(p, jj, e, h, index, LEFT).wait_send()

    each(SIDE, drain)


def gather(new, moments):
    copies = 90
    wide, tall = (10, 2, 3200), (50, 2, 640)
    outs = [pltpu.VMEM((2, 640, 3200), BF)] * 2 + [pltpu.VMEM((2, 3200, 640), BF)]
    outs += [pltpu.VMEM(one, F32) for one in (wide, wide, tall)] * 2
    return pl.pallas_call(
        gather_kernel,
        out_shape=outs,
        in_specs=[VM] * 4,
        out_specs=[VM] * MANY,
        scratch_shapes=[
            *halves(*GRID) * 3,
            pltpu.SemaphoreType.DMA((copies,)),
            pltpu.SemaphoreType.DMA((copies,)),
            pltpu.SemaphoreType.DMA((3, 4, 6)),
            pltpu.SemaphoreType.DMA((3, 4, 6)),
        ],
        compiler_params=pltpu.CompilerParams(collective_id=1, has_side_effects=True, vmem_limit_bytes=30 * 2**20),
        name="gather",
    )(*new, *moments)


def finish_kernel(*refs):
    held, outs, sem = refs[:MANY], refs[MANY : 2 * MANY], refs[2 * MANY]
    copies = [pltpu.make_async_copy(a, b, sem.at[n]) for n, (a, b) in enumerate(zip(held, outs))]
    for c in copies:
        c.start()
    for c in copies:
        c.wait()


def finish(held):
    return pl.pallas_call(
        finish_kernel,
        out_shape=[shape(*one.shape, dtype=one.dtype) for one in held],
        in_specs=[VM] * MANY,
        out_specs=[ANY] * MANY,
        scratch_shapes=[pltpu.SemaphoreType.DMA((MANY,))],
        compiler_params=pltpu.CompilerParams(vmem_limit_bytes=8 * 2**20),
        name="finish",
    )(*held)


def solution(mesh):
    def run(*arrays):
        terms, weights, m, v = (arrays[i : i + 3] for i in (0, 3, 6, 9))
        swap = lambda arrays: [x.transpose(1, 0, 2) for x in arrays]
        *new, mo, vo = step([t[0] for t in terms], weights, swap(m), swap(v))
        outs = finish(gather(new, (mo, vo)))
        return (*outs[:3], *swap(outs[3:]))

    all_of, cut = P(None, None, None), P(None, "dp", None)
    return jax.shard_map(
        run,
        mesh=mesh,
        in_specs=(P(("rep", "dp"), None, None, None),) * 3 + (all_of,) * 3 + (cut,) * 6,
        out_specs=(P("rep", None, None),) * 3 + (P("rep", "dp", None),) * 6,
        check_vma=False,
    )
```

```python
import jax
import jax.numpy as jnp
from jax import lax
from jax.experimental import pallas as pl
from jax.experimental.pallas import tpu as pltpu
from jax.sharding import PartitionSpec as P

MESH = pl.DeviceIdType.MESH
BF, F32 = jnp.bfloat16, jnp.float32
ANY = pl.BlockSpec(memory_space=pl.ANY)
VM = pl.BlockSpec(memory_space=pltpu.VMEM)
LANES = 128
X, Y, Z = range(3)
FIRST, SECOND, THIRD = range(3)
LEFT, RIGHT, FAR, ME = -1, 1, 2, 0
LAYERS = (0, 1)
COUNT = 3 * 2 * 640 * 3200

ROWS = 504
HALF = (256, 248)
SPAN = (pl.ds(0, 256), pl.ds(256, 248))
QUAD, TAIL = 80, 24
GROUPS = [range(t, min(t + 4, 25)) for t in range(0, 25, 4)]
ORDERS = ((X, Y, Z), (Y, Z, X), (Z, X, Y))
PARTS = range(3)
MANY = 9
LAG = 3
ORDER = (ME, LEFT, RIGHT, FAR)
SIDE, RING, GRID = 4, range(4), (4, 4, 4)


def wide_rows(tile, layer):
    return tile * 20 + layer * 10


def tall_rows(tile, layer):
    return tile * 100 + layer * 50


def stack(values, axis=0):
    return jnp.concatenate(values, axis=axis)


def put(out, z, first, value):
    cut = HALF[0]
    end = first + value.shape[0]
    value = value.astype(BF) if first >= cut or end <= cut else value
    if first >= cut:
        out[1][z, first - cut : end - cut, :] = value
    elif end <= cut:
        out[0][z, first:end, :] = value
    else:
        out[0][z, first:cut, :] = value[: cut - first].astype(BF)
        out[1][z, : end - cut, :] = value[cut - first :].astype(BF)


def get(ref, z, first, end):
    cut = HALF[0]
    low, high = first // 16 * 16, -(-end // 16) * 16
    if low >= cut:
        value = ref[1][z, low - cut : min(high, ROWS) - cut, :].astype(F32)
    elif high <= cut:
        value = ref[0][z, low:high, :].astype(F32)
    else:
        value = stack([ref[0][z, low:cut, :].astype(F32), ref[1][z, : min(high, ROWS) - cut, :].astype(F32)])
    return value[first - low : end - low]


def pack_wide(src, out):
    for group in range(7):
        tiles = GROUPS[group]
        x = [[src[s, :, pl.ds(t * LANES, LANES)].astype(F32) for s in LAYERS] for t in tiles]
        for z in RING:
            rows = [one[s][z * 10 : (z + 1) * 10] for one in x for s in LAYERS]
            if len(tiles) == 1:
                rows.append(jnp.zeros((SIDE, LANES), F32))
            put(out, z, group * QUAD, stack(rows))


def unpack_wide(block, write):
    for group in range(7):
        tiles = GROUPS[group]
        got = [get(block, z, group * QUAD, min(ROWS, (group + 1) * QUAD)) for z in RING]
        for n, t in enumerate(tiles):
            for s in LAYERS:
                row = n * 20 + s * 10
                write(s, pl.ds(t * LANES, LANES), stack([one[row : row + 10] for one in got]))


def pack_tall(src, out):
    x = [[src[s, :, pl.ds(t * LANES, LANES)].astype(F32) for s in LAYERS] for t in range(5)]
    for z in RING:
        rows = [one[s][z * 50 : (z + 1) * 50] for one in x for s in LAYERS]
        put(out, z, 0, stack([*rows, jnp.zeros((SIDE, LANES), F32)]))


def unpack_tall(block, write):
    got = [get(block, z, 0, ROWS) for z in RING]
    for t in range(5):
        for s in LAYERS:
            row = tall_rows(t, s)
            write(s, pl.ds(t * LANES, LANES), stack([one[row : row + 50] for one in got]))


def each(count, body, start=0):
    lax.fori_loop(start, count, lambda i, _: (body(i), None)[1], None)


class Part:
    pass


class Place:
    def __init__(self, partners, other_core=False):
        self.rep, dp = lax.axis_index("rep"), lax.axis_index("dp")
        self.here = (lax.div(dp, 16), lax.rem(lax.div(dp, 4), 4), lax.rem(dp, 4))
        barrier = pltpu.get_barrier_semaphore()
        for axis in (X, Y, Z):
            for by in partners:
                pl.semaphore_signal(barrier, inc=1, device_id=self.device(axis, by), device_id_type=MESH)
        if other_core:
            pl.semaphore_signal(barrier, inc=1, device_id=self.other_core(), device_id_type=MESH)
        self.barrier, self.greeted = barrier, 3 * len(partners) + other_core
        self.count = 0
        self.started = []

    def at(self, axis, by):
        return lax.rem(self.here[axis] + (by + 4), 4)

    def device(self, axis, by):
        c = [self.at(a, by if a == axis else ME) for a in (X, Y, Z)]
        return (self.rep, c[X] * 16 + c[Y] * 4 + c[Z])

    def wait(self):
        pl.semaphore_wait(self.barrier, self.greeted)

    def other_core(self):
        c = self.here
        return (1 - self.rep, c[X] * 16 + c[Y] * 4 + c[Z])

    def copy(self, src, dst, axis, by, send, recv):
        return pltpu.make_async_remote_copy(
            src_ref=src, dst_ref=dst, send_sem=send, recv_sem=recv, device_id=self.device(axis, by), device_id_type=MESH
        )

    def send(self, src, dst, axis, by, sems):
        copy = self.copy(src, dst, axis, by, sems[0].at[self.count], sems[1].at[self.count])
        self.count += 1
        copy.start()
        self.started.append(copy)
        return copy

    def parts(self):
        made = []
        for n in PARTS:
            p = Part()
            p.n, p.order = n, ORDERS[n]
            p.second = ORDERS[n][SECOND] < ORDERS[n][THIRD]
            made.append(p)
        return made

    def index(self, p, i, j, k):
        index = [None] * 3
        for a, value in zip(p.order, (i, j, k)):
            index[a] = slice(None) if value is None else value
        return tuple(index)


def step_kernel(*refs):
    grads, weights, m_in, v_in = (refs[i : i + 3] for i in (0, 3, 6, 9))
    new0, new1, mo, vo = refs[12:16]
    scratch = refs[16:]
    lines, scratch = scratch[:3], scratch[3:]
    own, scratch = [scratch[2 * n : 2 * n + 2] for n in PARTS], scratch[6:]
    packed, scratch = [scratch[2 * n : 2 * n + 2] for n in PARTS], scratch[6:]
    rec, scratch = [[scratch[18 * n + 6 * f : 18 * n + 6 * f + 6] for f in PARTS] for n in PARTS], scratch[54:]
    gs, sq, sqr, send, recv, early_send, early_recv, load_sem, go = scratch
    sems = (send, recv)

    place = Place((RIGHT, FAR, LEFT), True)
    ahead, behind = place.rep == 1, place.rep == 0
    at = place.at
    parts = place.parts()

    def line_copies(srcs, line, slot):
        for n, (src, height) in enumerate(zip(srcs, (40, 40, 200))):
            rows = pl.ds(pl.multiple_of(line * height, 8), height)
            yield pltpu.make_async_copy(src.at[:, rows, :], lines[n].at[slot], load_sem.at[slot, n])

    def pack(slot, outs):
        for n in PARTS:
            src = lines[n].at[slot]
            if n < 2:
                pack_wide(src, outs[n])
            else:
                pack_tall(src, outs[n])

    def distance(u):
        return lax.rem(6 - u + 3 * lax.div(u, 2) - 2 * lax.div(u, 3), 4)

    def where(t):
        u, w = lax.div(t, 4), lax.rem(t, 4)
        return w, lax.rem(u + w, 4)

    def line_of(t):
        a, b = where(t)
        return at(X, distance(a)), at(Y, distance(b))

    def start_line(t):
        x, y = line_of(t)
        for c in line_copies(grads, x * 4 + y, lax.rem(t, 2)):
            c.start()

    start_line(0)
    start_line(1)

    def early(p, s, src, dst, way):
        return place.copy(src, dst, p.order[FIRST], way, early_send.at[p.n, s], early_recv.at[p.n, s])

    def to_far(p, piece, block):
        for half, way in enumerate((RIGHT, LEFT)):
            early(p, half, packed[p.n][half].at[piece], rec[p.n][FIRST][half].at[block], way).start()

    def one_line(t, first=False):
        slot = lax.rem(t, 2)
        a, b = where(t)
        x, y = line_of(t)
        for c in line_copies(grads, x * 4 + y, slot):
            c.wait()
        pack(slot, [[half.at[x, y] for half in packed[n]] for n in PARTS])

        @pl.when(t < 14)
        def _():
            start_line(t + 2)

        if first:
            place.wait()

        @pl.when(a == 0)
        def _():
            to_far(parts[0], (x, y), y)

        @pl.when(b == 0)
        def _():
            to_far(parts[1], (x, y), x)

        to_far(parts[2], (x, y, at(Z, FAR)), (x, y))

    one_line(0, True)
    each(16, one_line, start=1)

    def whole_pieces(kinds):
        for p in parts:
            for s, half, by, way in kinds:
                piece = place.index(p, at(p.order[FIRST], by), None, None)
                early(p, s, packed[p.n][half].at[piece], rec[p.n][FIRST][s], way).start()

    NEAR_PIECES = ((2, 1, RIGHT, RIGHT), (3, 0, LEFT, LEFT))

    @pl.when(ahead)
    def _():
        whole_pieces(NEAR_PIECES)

    def early_sent():
        for p in parts:
            for s in RING:
                ref = rec[p.n][FIRST][s]
                early(p, s, ref, ref, LEFT).wait_send()

    for c in line_copies(weights, at(X, ME) * 4 + at(Y, ME), 0):
        c.start()
    for new, old in ((mo, m_in), (vo, v_in)):
        new[:, ROWS - TAIL : ROWS, :] = jnp.zeros((3, TAIL, LANES), F32)
        for n in PARTS:
            rows, height, tiles = (tall_rows, 50, 5) if n == 2 else (wide_rows, 10, 25)
            for tile in range(tiles):
                for s in LAYERS:
                    new[n, pl.ds(rows(tile, s), height), :] = old[n][:, s, tile * LANES : (tile + 1) * LANES]
    for c in line_copies(weights, at(X, ME) * 4 + at(Y, ME), 0):
        c.wait()
    pack(0, own)

    @pl.when(behind)
    def _():
        pl.semaphore_wait(go, 1)
        whole_pieces(NEAR_PIECES)

    def early_wait(p, s):
        ref = rec[p.n][FIRST][s]
        early(p, s, ref, ref, LEFT).wait_recv()

    def block(p, ref, j, k):
        return ref.at[(j, k) if p.second else (k, j)]

    def whole(p, ref, j):
        return ref.at[j] if p.second else ref.at[:, j]

    def total(refs):
        value = refs[0][...].astype(F32)
        for ref in refs[1:]:
            value = value + ref[...].astype(F32)
        return value

    def terms1(p, half, piece, j, k):
        return [packed[p.n][half].at[place.index(p, piece, j, k)]]

    def terms2(p, half, j, k):
        _, _, dir_l, dir_r, com_l, com_r = rec[p.n][FIRST]
        more = ((dir_r, com_l), (dir_l, com_r))[half]
        return terms1(p, half, p.me[FIRST], j, k) + [block(p, ref, j, k) for ref in more]

    def terms3(p, half, k):
        _, _, dir_l, dir_r, com_l, com_r = rec[p.n][SECOND]
        more = ((dir_r, com_l), (dir_l, com_r))[half]
        return terms2(p, half, p.me[SECOND], k) + [ref.at[k] for ref in more]

    STEPS = (FAR, RIGHT, LEFT, ME)
    LEAVES = {
        FAR: ((0, 3, 0, RIGHT), (1, 2, 1, LEFT)),
        RIGHT: ((1, 2, 2, RIGHT),),
        LEFT: ((0, 3, 3, LEFT),),
        ME: (),
    }
    COMBINE = ((0, 0, 4, RIGHT), (1, 1, 5, LEFT))

    for p in parts:
        p.me = [at(a, ME) for a in p.order]
        p.to = {by: [at(a, by) for a in p.order] for by in STEPS}
        early_wait(p, 0)
        early_wait(p, 1)
        p.com = {}
    for by in STEPS:
        for p in parts:
            j = p.to[by][SECOND]
            p.com[by] = []
            for half, got, to, way in COMBINE:
                got, to = (rec[p.n][FIRST][i] for i in (got, to))

                def add(k):
                    ref = block(p, got, j, k)
                    ref[...] = total(terms1(p, half, p.to[way][FIRST], j, k) + [ref]).astype(BF)

                each(SIDE, add)
                p.com[by].append(place.send(whole(p, got, j), whole(p, to, j), p.order[FIRST], way, sems))

    @pl.when(ahead)
    def _():
        early_sent()
        for c in place.started:
            c.wait_send()
        pl.semaphore_signal(go, inc=1, device_id=place.other_core(), device_id_type=MESH)

    for p in parts:
        early_wait(p, 2)
        early_wait(p, 3)
        p.next = {}

    for by in STEPS:
        for p in parts:
            j = p.to[by][SECOND]
            for c in p.com[by]:
                c.wait_recv()
            for half, slot, target, way in LEAVES[by]:
                ref = rec[p.n][FIRST][slot]

                def add(k):
                    block(p, ref, j, k)[...] = total(terms2(p, half, j, k)).astype(BF)

                each(SIDE, add)
                p.next[target] = place.send(whole(p, ref, j), rec[p.n][SECOND][target], p.order[SECOND], way, sems)

    for p in parts:
        p.next[0].wait_recv()
        p.next[1].wait_recv()
    for by in STEPS:
        for p in parts:
            k = p.to[by][THIRD]
            p.com[by] = []
            for half, got, to, way in COMBINE:
                got, to = (rec[p.n][SECOND][i].at[k] for i in (got, to))
                got[...] = total(terms2(p, half, p.to[way][SECOND], k) + [got]).astype(BF)
                p.com[by].append(place.send(got, to, p.order[SECOND], way, sems))
    for p in parts:
        p.next[2].wait_recv()
        p.next[3].wait_recv()
        p.next = {}

    for by in STEPS:
        for p in parts:
            k = p.to[by][THIRD]
            for c in p.com[by]:
                c.wait_recv()
            for half, slot, target, way in LEAVES[by]:
                ref = rec[p.n][SECOND][slot].at[k]
                ref[...] = total(terms3(p, half, k)).astype(BF)
                p.next[target] = place.send(ref, rec[p.n][THIRD][target], p.order[THIRD], way, sems)

    for p in parts:
        p.com = []
        for half, got, to, way in COMBINE:
            p.next[got].wait_recv()
            got, to = (rec[p.n][THIRD][i] for i in (got, to))
            got[...] = total(terms3(p, half, p.to[way][THIRD]) + [got]).astype(BF)
            p.com.append(place.send(got, to, p.order[THIRD], way, sems))
    squares = jnp.zeros((8, LANES), F32)
    for p in parts:
        for c in (p.next[2], p.next[3], *p.com):
            c.wait_recv()
        _, _, dir_l, dir_r, com_l, com_r = rec[p.n][THIRD]
        for half in LAYERS:
            g = total(terms3(p, half, p.me[THIRD]) + [(dir_r, dir_l)[half], (com_l, com_r)[half]]).astype(BF).astype(F32)
            gs[p.n, SPAN[half], :] = g
            squares += jnp.sum((g * g).reshape(-1, 8, LANES), axis=0)

    for axis in (X, Y, Z):
        sq[axis] = squares
        copies = [place.send(sq.at[axis], sqr.at[axis, i], axis, by, sems) for i, by in enumerate((RIGHT, FAR, LEFT))]
        for i, c in enumerate(copies):
            c.wait_recv()
            squares += sqr[axis, i]
    squares = jnp.sum(squares, axis=(0, 1), keepdims=True)
    factor = jnp.minimum(1.0, 0.5 * lax.rsqrt(squares / COUNT + 1e-30))

    for n in PARTS:
        for half in LAYERS:
            rows = SPAN[half]
            g = gs[n, rows, :] * factor
            w = own[n][half][at(Z, ME)].astype(F32)
            m = 0.9 * mo[n, rows, :] + 0.1 * g
            v = 0.95 * vo[n, rows, :] + 0.05 * g * g
            mo[n, rows, :] = m
            vo[n, rows, :] = v
            (new0, new1)[half][n] = (w - 0.02 * (m * lax.rsqrt(v + 1e-8) + 0.1 * w)).astype(BF)

    for c in place.started[24:]:
        c.wait_send()

    @pl.when(behind)
    def _():
        early_sent()
        for c in place.started[:24]:
            c.wait_send()


def halves(*lead, dtype=BF):
    return [pltpu.VMEM((*lead, h, LANES), dtype) for h in HALF]


def shape(*dims, dtype=BF):
    return jax.ShapeDtypeStruct(dims, dtype)


def step(grads, weights, m, v):
    rec = []
    for lead in ((4, 4), (4,), ()):
        a, b = halves(*lead)
        rec += [a, b, b, a, a, b]
    copies = 87
    return pl.pallas_call(
        step_kernel,
        out_shape=[shape(3, HALF[0], LANES), shape(3, HALF[1], LANES)] + [shape(3, ROWS, LANES, dtype=F32)] * 2,
        in_specs=[ANY] * 6 + [VM] * 6,
        out_specs=[VM] * 4,
        scratch_shapes=[
            pltpu.VMEM((2, 2, 40, 3200), BF),
            pltpu.VMEM((2, 2, 40, 3200), BF),
            pltpu.VMEM((2, 2, 200, 640), BF),
            *halves(4) * 3,
            *halves(*GRID) * 3,
            *rec * 3,
            pltpu.VMEM((3, ROWS, LANES), F32),
            pltpu.VMEM((3, 8, LANES), F32),
            pltpu.VMEM((3, 3, 8, LANES), F32),
            pltpu.SemaphoreType.DMA((copies,)),
            pltpu.SemaphoreType.DMA((copies,)),
            pltpu.SemaphoreType.DMA((3, 4)),
            pltpu.SemaphoreType.DMA((3, 4)),
            pltpu.SemaphoreType.DMA((2, 3)),
            pltpu.SemaphoreType.REGULAR,
        ],
        compiler_params=pltpu.CompilerParams(collective_id=0, has_side_effects=True, vmem_limit_bytes=67043328),
        name="step",
    )(*grads, *weights, *m, *v)


def gather_kernel(*refs):
    new, moments, outs, moved = (refs[i:j] for i, j in ((0, 2), (2, 4), (4, 7), (7, 13)))
    scratch = refs[13:]
    got = [scratch[2 * n : 2 * n + 2] for n in PARTS]
    send, recv, late_send, late_recv = scratch[6:]
    sems = (send, recv)

    place = Place((RIGHT, LEFT))
    at = place.at
    parts = place.parts()
    for p in parts:
        p.me, p.left, p.right, p.far = ([at(a, by) for a in p.order] for by in (ME, LEFT, RIGHT, FAR))
        p.steps = (p.me, p.left, p.right, p.far)

    def ref_of(p, half, i, j, k):
        return got[p.n][half].at[place.index(p, i, j, k)]

    def spread(p, axis, i, j, k, mine=False):
        to = [ref_of(p, h, i, j, k) for h in LAYERS]
        src = [new[h].at[p.n] for h in LAYERS] if mine else to
        return [place.send(src[h], to[h], axis, by, sems) for h, by in ((0, RIGHT), (1, LEFT), (1, RIGHT), (0, LEFT))]

    def forward(p, axis, copies, from_left, from_right):
        copies[0].wait_recv()
        left = ref_of(p, 0, *from_left)
        a = place.send(left, left, axis, RIGHT, sems)
        copies[1].wait_recv()
        right = ref_of(p, 1, *from_right)
        return a, place.send(right, right, axis, LEFT, sems)

    def arrived(*copies):
        for c in copies:
            c.wait_recv()

    def chunk(p, axis_place, step):
        i, value = axis_place, step
        return (i, None, value) if p.n == 1 else (i, value, None)

    def late(p, jj, e, half, index, way):
        ref = ref_of(p, half, *index)
        return place.copy(ref, ref, p.order[FIRST], way, late_send.at[p.n, jj, e], late_recv.at[p.n, jj, e])

    def along(p):
        return p.order[THIRD if p.n == 1 else SECOND]

    def last_spread(p, j, k):
        jj = ORDER.index(k if p.n == 1 else j)
        mine = j == ME and k == ME
        index = (p.me[FIRST], at(p.order[SECOND], j), at(p.order[THIRD], k))
        for e, (h, way) in enumerate(((0, RIGHT), (1, LEFT), (1, RIGHT), (0, LEFT))):
            to = ref_of(p, h, *index)
            sems = late_send.at[p.n, jj, e], late_recv.at[p.n, jj, e]
            place.copy(new[h].at[p.n] if mine else to, to, p.order[FIRST], way, *sems).start()

    for p in parts:
        for h in LAYERS:
            ref_of(p, h, *p.me)[...] = new[h][p.n]
    place.wait()

    for p in parts:
        p.s3 = spread(p, p.order[THIRD], *p.me, mine=True)
    for p in parts:
        p.s2, p.f2 = [spread(p, p.order[SECOND], *p.me, mine=True)], []
    for p in parts:
        last_spread(p, ME, ME)
    for p in parts:
        i, j, k = p.me
        p.f3 = forward(p, p.order[THIRD], p.s3, (i, j, p.left[THIRD]), (i, j, p.right[THIRD]))
    for p in parts:
        arrived(*p.s3[2:])
        for k in (p.left[THIRD], p.right[THIRD]):
            p.s2.append(spread(p, p.order[SECOND], *p.me[:THIRD], k))
    for p in parts:
        last_spread(p, ME, LEFT)
        last_spread(p, ME, RIGHT)
    for p in parts:
        arrived(*p.f3)
        p.s2.append(spread(p, p.order[SECOND], *p.me[:THIRD], p.far[THIRD]))
        last_spread(p, ME, FAR)
    for step, by in enumerate((*ORDER, None)):
        for p in parts:
            if by is not None:
                i, k = p.me[FIRST], p.steps[step][THIRD]
                p.f2.append(forward(p, p.order[SECOND], p.s2[step], (i, p.left[SECOND], k), (i, p.right[SECOND], k)))
        for p in parts:
            if by is not None:
                arrived(*p.s2[step][2:])
                last_spread(p, LEFT, by)
                last_spread(p, RIGHT, by)
            if step:
                arrived(*p.f2[step - 1])
                last_spread(p, FAR, ORDER[step - 1])

    for out, one in zip((moved[:3], moved[3:]), moments):
        for n in PARTS:
            rows, height, tiles = (tall_rows, 50, 5) if n == 2 else (wide_rows, 10, 25)
            for tile in range(tiles):
                for s in LAYERS:
                    out[n][:, s, tile * LANES : (tile + 1) * LANES] = one[n, pl.ds(rows(tile, s), height), :]


    def line(p, x, y):
        block = [half.at[x, y] for half in got[p.n]]
        height = 200 if p.n == 2 else 40
        rows = pl.ds(pl.multiple_of((x * 4 + y) * height, 8), height)

        def write(layer, columns, value):
            outs[p.n][layer, rows, columns] = value.astype(BF)

        if p.n == 2:
            unpack_tall(block, write)
        else:
            unpack_wide(block, write)

    def distance(jj):
        return 3 * lax.rem(jj, 2) + lax.div(jj, 2) - 2 * lax.div(jj, 3)

    def last(jj):
        @pl.when(jj < 4)
        def _():
            for p in parts:
                value = at(along(p), distance(jj))
                left, right = (chunk(p, i, value) for i in (p.left[FIRST], p.right[FIRST]))
                late(p, jj, 0, 0, left, LEFT).wait_recv()
                late(p, jj, 4, 0, left, RIGHT).start()
                late(p, jj, 1, 1, right, LEFT).wait_recv()
                late(p, jj, 5, 1, right, LEFT).start()
            for p in parts:
                value = at(along(p), distance(jj))
                left, right = (chunk(p, i, value) for i in (p.left[FIRST], p.right[FIRST]))
                late(p, jj, 2, 1, left, LEFT).wait_recv()
                late(p, jj, 3, 0, right, LEFT).wait_recv()

        before = jj - LAG

        @pl.when(jj >= LAG)
        def _():
            for p in parts:
                far = chunk(p, p.far[FIRST], at(along(p), distance(before)))
                late(p, before, 4, 0, far, LEFT).wait_recv()
                late(p, before, 5, 1, far, LEFT).wait_recv()

        def one(i):
            which = jj - LAG * lax.div(i, 3)

            @pl.when((which >= 0) & (which < 4))
            def _():
                value = distance(which)
                line(parts[0], at(X, distance(i)), at(Y, value))
                line(parts[1], at(X, value), at(Y, distance(i)))

            @pl.when(jj >= LAG)
            def _():
                line(parts[2], at(X, distance(before)), i)

        each(SIDE, one)

    each(SIDE + LAG, last)

    for c in place.started:
        c.wait_send()

    def drain(jj):
        for p in parts:
            index = chunk(p, p.me[FIRST], at(along(p), distance(jj)))
            for e, h in enumerate((0, 1, 1, 0, 0, 1)):
                late(p, jj, e, h, index, LEFT).wait_send()

    each(SIDE, drain)


def gather(new, moments):
    copies = 90
    wide, tall = (10, 2, 3200), (50, 2, 640)
    outs = [pltpu.VMEM((2, 640, 3200), BF)] * 2 + [pltpu.VMEM((2, 3200, 640), BF)]
    outs += [pltpu.VMEM(one, F32) for one in (wide, wide, tall)] * 2
    return pl.pallas_call(
        gather_kernel,
        out_shape=outs,
        in_specs=[VM] * 4,
        out_specs=[VM] * MANY,
        scratch_shapes=[
            *halves(*GRID) * 3,
            pltpu.SemaphoreType.DMA((copies,)),
            pltpu.SemaphoreType.DMA((copies,)),
            pltpu.SemaphoreType.DMA((3, 4, 6)),
            pltpu.SemaphoreType.DMA((3, 4, 6)),
        ],
        compiler_params=pltpu.CompilerParams(collective_id=1, has_side_effects=True, vmem_limit_bytes=30 * 2**20),
        name="gather",
    )(*new, *moments)


def finish_kernel(*refs):
    held, outs, sem = refs[:MANY], refs[MANY : 2 * MANY], refs[2 * MANY]
    copies = [pltpu.make_async_copy(a, b, sem.at[n]) for n, (a, b) in enumerate(zip(held, outs))]
    for c in copies:
        c.start()
    for c in copies:
        c.wait()


def finish(held):
    return pl.pallas_call(
        finish_kernel,
        out_shape=[shape(*one.shape, dtype=one.dtype) for one in held],
        in_specs=[VM] * MANY,
        out_specs=[ANY] * MANY,
        scratch_shapes=[pltpu.SemaphoreType.DMA((MANY,))],
        compiler_params=pltpu.CompilerParams(vmem_limit_bytes=8 * 2**20),
        name="finish",
    )(*held)


def solution(mesh):
    def run(*arrays):
        terms, weights, m, v = (arrays[i : i + 3] for i in (0, 3, 6, 9))
        swap = lambda arrays: [x.transpose(1, 0, 2) for x in arrays]
        *new, mo, vo = step([t[0] for t in terms], weights, swap(m), swap(v))
        outs = finish(gather(new, (mo, vo)))
        return (*outs[:3], *swap(outs[3:]))

    all_of, cut = P(None, None, None), P(None, "dp", None)
    return jax.shard_map(
        run,
        mesh=mesh,
        in_specs=(P(("rep", "dp"), None, None, None),) * 3 + (all_of,) * 3 + (cut,) * 6,
        out_specs=(P("rep", None, None),) * 3 + (P("rep", "dp", None),) * 6,
        check_vma=False,
    )
```
